128 devices in a mesh: zone: 8 (over x, y_lo), dev: 16 (over y_hi, z, core).
Axes of the slice: x: 4, y: 4 (y_hi: 2, y_lo: 2; y = y_hi * 2 + y_lo), z: 4, core: 2. Of those that a mesh axis runs over, the one named last changes fastest.
Arguments:
- node_features: bfloat16 [65536, 512], P(('zone', 'dev')), may hold values from -9 to 9
- neighbour_blocks: int32 [512, 32], P(('zone', 'dev')), may hold values from 0 to 511, as said below
- neighbour_count: int32 [512], P(('zone', 'dev')), may hold values from 8 to 32, as said below
- tile_valid: int32 [512], replicated, may hold values from 64 to 128
- w_query: bfloat16 [512, 512], replicated, may hold values from -0.5 to 0.5
- w_key: bfloat16 [512, 512], replicated, may hold values from -0.5 to 0.5
- w_value: bfloat16 [512, 512], replicated, may hold values from -0.25 to 0.25
- w_out: bfloat16 [512, 512], replicated, may hold values from -0.25 to 0.25
- w_gate: bfloat16 [512, 2048], replicated, may hold values from -0.25 to 0.25
- w_up: bfloat16 [512, 2048], replicated, may hold values from -0.25 to 0.25
- w_down: bfloat16 [2048, 512], replicated, may hold values from -0.125 to 0.125
Outputs:
- layer_out: bfloat16 [65536, 512], P(('zone', 'dev'))
The draws below stay inside these ranges and needn't reach their ends.
Inputs may be any that keep to these rules, and one draw needn't show every extreme that they name: `neighbour_blocks`: each row lists 32 different blocks. Zones are runs of 64 blocks (zone of block g is g // 64); every listed block lies in the query block's zone or in one of the two zones beside it, counting around the last zone to the first. Each value is 8, 16 or 32, one value for each patch of 16 consecutive blocks (patch of block g is g // 16); only the first neighbour_count[b] slots of row b count.
All inputs are finite; a program needn't handle non-finite values.
Results may differ from the reference program's by a relative error of at most 0.007.
The reference program's roundings to bfloat16 on the way count: a program that leaves them out, or rounds other values in their place, can miss the bound.
Values may be sent and summed in bfloat16 or wider, within the bound.
A program may use at most 448 MiB of HBM per device.

```python
import math
import jax
import jax.numpy as jnp
from jax import lax

D = 512
HEADS = 4
FF = 2048
TILE = 128
NB = 32
BLK_DEV = 4
BLOCKS = 512
NODES = 65536
N_ZONE = 8
N_DEV = 16


def draw_node_features(key, part):
    normal_part = jax.random.normal(jax.random.fold_in(key, 3), (NODES, D), jnp.float32)
    return jnp.clip(normal_part, -6.0, 6.0).astype(jnp.bfloat16)


def draw_neighbour_blocks(key, part):
    zone_blocks = BLK_DEV * N_DEV
    span = 3 * zone_blocks
    row_keys = jax.random.split(jax.random.fold_in(key, 11), BLOCKS)
    chosen = jax.vmap(lambda row_key: jax.random.permutation(row_key, span)[:NB])(row_keys)
    owner_zone = (jnp.arange(BLOCKS, dtype=jnp.int32) // zone_blocks)[:, None]
    zone_index = (owner_zone - 1 + chosen // zone_blocks) % N_ZONE
    return (zone_index * zone_blocks + chosen % zone_blocks).astype(jnp.int32)


def draw_neighbour_count(key, part):
    patch_blocks = 4 * BLK_DEV
    patch_total = BLOCKS // patch_blocks
    level_key, order_key = jax.random.split(jax.random.fold_in(key, 7))
    level = jax.random.randint(level_key, (patch_total,), 0, 3)
    order = jax.random.permutation(order_key, patch_total)
    level = level.at[order[0]].set(2).at[order[1]].set(0)
    counts = jnp.where(level == 0, NB // 4, jnp.where(level == 1, NB // 2, NB))
    return jnp.repeat(counts, patch_blocks).astype(jnp.int32)


def plant(values, own_key, smallest, top_value):
    index_at = [jax.random.randint(jax.random.fold_in(own_key, axis), (), 0, length) for axis, length in enumerate(values.shape)]
    widest = values.shape.index(max(values.shape))
    next_to = index_at[:widest] + [(index_at[widest] + 1) % values.shape[widest]] + index_at[widest + 1:]
    return values.at[tuple(index_at)].set(smallest).at[tuple(next_to)].set(top_value)


def noise(stream_key, dims, spread, bound, kind=jnp.bfloat16):
    values = jax.random.normal(stream_key, dims, jnp.float32) * spread
    return jnp.minimum(jnp.maximum(values, -bound), bound).astype(kind)


def setup_inputs(seed: int = 0) -> dict:
    splits = jax.random.split(jax.random.key(seed), 12)
    node_features = draw_node_features(jax.random.fold_in(splits[11], 71), 0)
    neighbour_blocks = draw_neighbour_blocks(jax.random.fold_in(splits[11], 71), 0)
    neighbour_count = draw_neighbour_count(jax.random.fold_in(splits[11], 71), 0)
    tile_valid = plant(jax.random.randint(splits[3], (BLOCKS,), TILE // 2, TILE + 1), jax.random.fold_in(splits[3], 1), TILE // 2, TILE).astype(jnp.int32)
    w_query = noise(splits[4], (D, D), (D // 4) ** -0.5, 0.5)
    w_key = noise(splits[5], (D, D), (D // 4) ** -0.5, 0.5)
    w_value = noise(splits[6], (D, D), D ** -0.5, 0.25)
    w_out = noise(splits[7], (D, D), D ** -0.5, 0.25)
    w_gate = noise(splits[8], (D, FF), D ** -0.5, 0.25)
    w_up = noise(splits[9], (D, FF), D ** -0.5, 0.25)
    w_down = noise(splits[10], (FF, D), FF ** -0.5, 0.125)
    return {"node_features": node_features, "neighbour_blocks": neighbour_blocks, "neighbour_count": neighbour_count, "tile_valid": tile_valid, "w_query": w_query, "w_key": w_key, "w_value": w_value, "w_out": w_out, "w_gate": w_gate, "w_up": w_up, "w_down": w_down}


def finish_layer(node_features, attended, w_out, w_gate, w_up, w_down):
    residual = node_features.astype(jnp.float32) + jnp.dot(attended, w_out, preferred_element_type=jnp.float32)
    inverse = lax.rsqrt(lax.optimization_barrier(jnp.mean(residual * residual, axis=-1, keepdims=True)) + 1e-06)
    normed = (residual * inverse).astype(jnp.bfloat16)
    gate_part = jnp.dot(normed, w_gate, preferred_element_type=jnp.float32)
    up_part = jnp.dot(normed, w_up, preferred_element_type=jnp.float32)
    hidden = (jax.nn.silu(gate_part) * up_part).astype(jnp.bfloat16)
    return (residual + jnp.dot(hidden, w_down, preferred_element_type=jnp.float32)).astype(jnp.bfloat16)

def reference(node_features, neighbour_blocks, neighbour_count, tile_valid, w_query, w_key, w_value, w_out, w_gate, w_up, w_down):
    head_dim = D // HEADS
    score_scale = 1.0 / math.sqrt(head_dim)
    queries = jnp.dot(node_features, w_query, preferred_element_type=jnp.float32).astype(jnp.bfloat16)
    key_rows = jnp.dot(node_features, w_key, preferred_element_type=jnp.float32).astype(jnp.bfloat16)
    value_rows = jnp.dot(node_features, w_value, preferred_element_type=jnp.float32).astype(jnp.bfloat16)
    queries, key_rows, value_rows = lax.optimization_barrier((queries, key_rows, value_rows))
    key_tiles = key_rows.reshape(BLOCKS, TILE, D)
    value_tiles = value_rows.reshape(BLOCKS, TILE, D)
    query_tiles = queries.reshape(BLOCKS, TILE, HEADS, head_dim)
    row_index = jnp.arange(TILE, dtype=jnp.int32)
    slot_index = jnp.arange(NB, dtype=jnp.int32)

    def one_block(block_item):
        query_tile, listed, live_count = block_item
        block_keys = jnp.take(key_tiles, listed, axis=0).reshape(NB * TILE, HEADS, head_dim).astype(jnp.float32)
        block_values = jnp.take(value_tiles, listed, axis=0).reshape(NB * TILE, HEADS, head_dim).astype(jnp.float32)
        valid_rows = jnp.take(tile_valid, listed)
        key_live = (slot_index < live_count)[:, None] & (row_index[None, :] < valid_rows[:, None])
        key_mask = key_live.reshape(1, 1, NB * TILE)
        scores = jnp.einsum('qhd,khd->hqk', query_tile.astype(jnp.float32), block_keys) * score_scale
        peak = lax.optimization_barrier(jnp.max(jnp.where(key_mask, scores, -1e+30), axis=-1, keepdims=True))
        weights = jnp.where(key_mask, jnp.exp(scores - peak), 0.0)
        denominator = lax.optimization_barrier(jnp.sum(weights, axis=-1))
        rounded = lax.optimization_barrier(weights.astype(jnp.bfloat16))
        summed = jnp.einsum('hqk,khd->qhd', rounded.astype(jnp.float32), block_values)
        return (summed / jnp.transpose(denominator)[:, :, None]).reshape(TILE, D).astype(jnp.bfloat16)
    attended = lax.map(one_block, (query_tiles, neighbour_blocks, neighbour_count)).reshape(NODES, D)
    return finish_layer(node_features, attended, w_out, w_gate, w_up, w_down)
```

```python
import functools
import math

import jax
import jax.numpy as jnp
from jax import lax
from jax.experimental import pallas as pl
from jax.experimental.pallas import tpu as pltpu
from jax.sharding import PartitionSpec as P

D = 512
HEADS = 4
HD = 128
TILE = 128
NB = 32
ZD = 4
NEG = -1e30
EXP_SCALE = math.log2(math.e) / math.sqrt(HD)


def proj_kernel(x_ref, wq_ref, wk_ref, wv_ref, q_ref, kv_ref):
    def one_tile(t, carry):
        x = x_ref[pl.ds(pl.multiple_of(t * TILE, TILE), TILE), :]
        q = jnp.dot(x, wq_ref[...], preferred_element_type=jnp.float32).astype(jnp.bfloat16)
        for h in range(HEADS):
            q_ref[h, t] = q[:, h * HD:(h + 1) * HD]
        k = jnp.dot(x, wk_ref[...], preferred_element_type=jnp.float32)
        for h in range(HEADS):
            kv_ref[h, t, 0] = jnp.transpose(k[:, h * HD:(h + 1) * HD]).astype(jnp.bfloat16)
        v = jnp.dot(x, wv_ref[...], preferred_element_type=jnp.float32).astype(jnp.bfloat16)
        for h in range(HEADS):
            kv_ref[h, t, 1] = v[:, h * HD:(h + 1) * HD]
        return carry

    lax.fori_loop(0, x_ref.shape[0] // TILE, one_tile, 0)


def project(x, wq, wk, wv):
    tiles = x.shape[0] // TILE
    return pl.pallas_call(
        proj_kernel,
        out_shape=(
            jax.ShapeDtypeStruct((HEADS, tiles, TILE, HD), jnp.bfloat16),
            jax.ShapeDtypeStruct((HEADS, tiles, 2, TILE, HD), jnp.bfloat16),
        ),
    )(x, wq, wk, wv)


def attn_kernel(code_ref, q_ref, kv_hbm, o_ref, kv_ref, s_ref, sem):
    chunks = 6
    step = kv_hbm.shape[0] // chunks
    copies = [
        pltpu.make_async_copy(
            kv_hbm.at[pl.ds(i * step, step)], kv_ref.at[pl.ds(i * step, step)], sem.at[i]
        )
        for i in range(chunks)
    ]
    for c in copies:
        c.start()
    for c in copies:
        c.wait()
    lane = lax.broadcasted_iota(jnp.int32, (1, TILE), 1)

    def one_tile(i, carry):
        groups = code_ref[i, NB] // 8
        q = q_ref[i]

        def scores(c, top):
            for p in range(4):
                a = code_ref[i, c * 8 + 2 * p]
                b = code_ref[i, c * 8 + 2 * p + 1]
                keys = jnp.concatenate([kv_ref[a // 256, 0], kv_ref[b // 256, 0]], axis=1)
                s = jnp.dot(q, keys, preferred_element_type=jnp.float32)
                bias = jnp.concatenate(
                    [
                        jnp.where(lane < a % 256, 0.0, NEG),
                        jnp.where(lane < b % 256, 0.0, NEG),
                    ],
                    axis=1,
                )
                s = s + bias
                s_ref[c, :, p * 256:(p + 1) * 256] = s
                top = jnp.maximum(top, jnp.maximum(s[:, :TILE], s[:, TILE:]))
            return top

        top = lax.fori_loop(0, groups, scores, jnp.full((TILE, TILE), NEG, jnp.float32))
        peak = jnp.max(top, axis=1, keepdims=True)

        def values(c, state):
            den, acc = state
            ps, vs = [], []
            for p in range(4):
                a = code_ref[i, c * 8 + 2 * p]
                b = code_ref[i, c * 8 + 2 * p + 1]
                w = jnp.exp2((s_ref[c, :, p * 256:(p + 1) * 256] - peak) * EXP_SCALE)
                den = den + (w[:, :TILE] + w[:, TILE:])
                ps.append(w.astype(jnp.bfloat16))
                vs += [kv_ref[a // 256, 1], kv_ref[b // 256, 1]]
            acc = acc + jnp.dot(
                jnp.concatenate(ps, axis=1),
                jnp.concatenate(vs, axis=0),
                preferred_element_type=jnp.float32,
            )
            return den, acc

        zero = jnp.zeros((TILE, TILE), jnp.float32)
        den, acc = lax.fori_loop(0, groups, values, (zero, zero))
        o_ref[i] = (acc / jnp.sum(den, axis=1, keepdims=True)).astype(jnp.bfloat16)
        return carry

    lax.fori_loop(0, q_ref.shape[0], one_tile, 0)


def attend(code, q, kv):
    return pl.pallas_call(
        attn_kernel,
        out_shape=jax.ShapeDtypeStruct(q.shape, jnp.bfloat16),
        in_specs=[
            pl.BlockSpec(memory_space=pltpu.SMEM),
            pl.BlockSpec(memory_space=pltpu.VMEM),
            pl.BlockSpec(memory_space=pl.ANY),
        ],
        out_specs=pl.BlockSpec(memory_space=pltpu.VMEM),
        scratch_shapes=[
            pltpu.VMEM(kv.shape, jnp.bfloat16),
            pltpu.VMEM((4, TILE, 8 * TILE), jnp.float32),
            pltpu.SemaphoreType.DMA((6,)),
        ],
        compiler_params=pltpu.CompilerParams(vmem_limit_bytes=40 * 1024 * 1024),
    )(code, q, kv)


def finish_layer(node_features, attended, w_out, w_gate, w_up, w_down):
    residual = node_features.astype(jnp.float32) + jnp.dot(
        attended, w_out, preferred_element_type=jnp.float32
    )
    inverse = lax.rsqrt(jnp.mean(residual * residual, axis=-1, keepdims=True) + 1e-06)
    normed = (residual * inverse).astype(jnp.bfloat16)
    gate_part = jnp.dot(normed, w_gate, preferred_element_type=jnp.float32)
    up_part = jnp.dot(normed, w_up, preferred_element_type=jnp.float32)
    hidden = (jax.nn.silu(gate_part) * up_part).astype(jnp.bfloat16)
    return (residual + jnp.dot(hidden, w_down, preferred_element_type=jnp.float32)).astype(
        jnp.bfloat16
    )


def make_codes(neighbour_blocks, neighbour_count, tile_valid, zone_blocks, zone_count):
    zone_index = lax.axis_index("zone")
    relative = (neighbour_blocks // zone_blocks - zone_index + 1) % zone_count
    local = neighbour_blocks % zone_blocks
    y_hi, rest = local // 32, local % 32
    z, rest = rest // 8, rest % 8
    core, t = rest // 4, rest % 4
    slot = (((relative * 2 + y_hi) * 2 + core) * ZD + z) * 4 + t
    matches = neighbour_blocks[..., None] == jnp.arange(tile_valid.shape[0], dtype=jnp.int32)
    valid = jnp.sum(jnp.where(matches, tile_valid, 0), axis=-1)
    live = jnp.arange(NB, dtype=jnp.int32)[None, :] < neighbour_count[:, None]
    code = slot * 256 + jnp.where(live, valid, 0)
    return jnp.concatenate(
        [code, neighbour_count[:, None], jnp.zeros((code.shape[0], 95), jnp.int32)], axis=1
    )


def body(
    x,
    neighbour_blocks,
    neighbour_count,
    tile_valid,
    w_query,
    w_key,
    w_value,
    w_out,
    w_gate,
    w_up,
    w_down,
):
    rows = x.shape[0]
    tiles = rows // TILE
    zone_count = lax.axis_size("zone")
    dev_count = lax.axis_size("dev")
    z_groups = [
        [y * 8 + z * 2 + c for z in range(ZD)] for y in range(2) for c in range(2)
    ]
    plane_groups = [
        [y * 8 + z * 2 + c for y in range(2) for c in range(2)] for z in range(ZD)
    ]
    codes = make_codes(
        neighbour_blocks, neighbour_count, tile_valid, tiles * dev_count, zone_count
    )
    q, kv = project(x, w_query, w_key, w_value)
    codes = lax.all_gather(codes, "dev", axis=0, axis_index_groups=z_groups, tiled=True)
    q = lax.all_to_all(q, "dev", 0, 0, axis_index_groups=z_groups, tiled=True)
    kv = lax.all_to_all(kv, "dev", 0, 0, axis_index_groups=z_groups, tiled=True)
    own = lax.all_gather(kv, "dev", axis=0, axis_index_groups=plane_groups)
    own = own.reshape(dev_count * tiles, 2, TILE, HD)
    ring = [(i, (i + 1) % zone_count) for i in range(zone_count)]
    before = lax.ppermute(own, "zone", ring)
    after = lax.ppermute(own, "zone", [(b, a) for a, b in ring])
    near = jnp.concatenate([before, own, after], axis=0)
    o = attend(codes, q.reshape(ZD * tiles, TILE, HD), near)
    o = lax.all_to_all(
        o.reshape(ZD, tiles, TILE, HD), "dev", 0, 0, axis_index_groups=z_groups, tiled=True
    )
    attended = jnp.transpose(o, (1, 2, 0, 3)).reshape(rows, D)
    return finish_layer(x, attended, w_out, w_gate, w_up, w_down)


def solution(mesh):
    placed = (
        P(("zone", "dev"), None),
        P(("zone", "dev"), None),
        P(("zone", "dev")),
        P(),
        P(),
        P(),
        P(),
        P(),
        P(),
        P(),
        P(),
    )
    return jax.shard_map(
        body, mesh=mesh, in_specs=placed, out_specs=P(("zone", "dev"), None), check_vma=False
    )
```

```python
import functools
import math

import jax
import jax.numpy as jnp
from jax import lax
from jax.experimental import pallas as pl
from jax.experimental.pallas import tpu as pltpu
from jax.sharding import PartitionSpec as P

D = 512
HEADS = 4
HD = 128
TILE = 128
NB = 32
ZD = 4
NEG = -1e30
EXP_SCALE = math.log2(math.e) / math.sqrt(HD)


def proj_kernel(x_ref, wq_ref, wk_ref, wv_ref, q_ref, kv_ref):
    def one_tile(t, carry):
        x = x_ref[pl.ds(pl.multiple_of(t * TILE, TILE), TILE), :]
        q = jnp.dot(x, wq_ref[...], preferred_element_type=jnp.float32).astype(jnp.bfloat16)
        for h in range(HEADS):
            q_ref[h, t] = q[:, h * HD:(h + 1) * HD]
        k = jnp.dot(x, wk_ref[...], preferred_element_type=jnp.float32)
        for h in range(HEADS):
            kv_ref[h, t, 0] = jnp.transpose(k[:, h * HD:(h + 1) * HD]).astype(jnp.bfloat16)
        v = jnp.dot(x, wv_ref[...], preferred_element_type=jnp.float32).astype(jnp.bfloat16)
        for h in range(HEADS):
            kv_ref[h, t, 1] = v[:, h * HD:(h + 1) * HD]
        return carry

    lax.fori_loop(0, x_ref.shape[0] // TILE, one_tile, 0)


def project(x, wq, wk, wv):
    tiles = x.shape[0] // TILE
    return pl.pallas_call(
        proj_kernel,
        out_shape=(
            jax.ShapeDtypeStruct((HEADS, tiles, TILE, HD), jnp.bfloat16),
            jax.ShapeDtypeStruct((HEADS, tiles, 2, TILE, HD), jnp.bfloat16),
        ),
    )(x, wq, wk, wv)


MESH = pl.DeviceIdType.MESH
DIRECT = 3
UP_SET = (0, 2)
DOWN_SET = (1, 3)


def exchange_kernel(code_ref, q_ref, kv_ref, code_out, q_out, kv_out, transit, send_sem, recv_sem):
    zone, dev = lax.axis_index("zone"), lax.axis_index("dev")
    x, y_lo = zone // 2, zone % 2
    y_hi, z, core = dev // 8, (dev // 2) % ZD, dev % 2
    y = y_hi * 2 + y_lo

    def at(px, py, pz, pc):
        return (px * 2 + py % 2, (py // 2) * 8 + pz * 2 + pc)

    side = 1 - 2 * y_lo
    up, down = at(x, (y + 1) % 4, z, core), at(x, (y + 3) % 4, z, core)
    halo, back = at((x + 4 + side) % 4, y, z, core), at((x + 4 - side) % 4, y, z, core)
    partner = at(x, y, z, 1 - core)
    z_at = [z] + [(z + d) % ZD for d in (1, 3, 2)]
    z_dev = [None] + [at(x, y, z_at[j], core) for j in (1, 2, 3)]

    barrier = pltpu.get_barrier_semaphore()
    peers = [up, down, halo, back, partner] + z_dev[1:]
    for peer in peers:
        pl.semaphore_signal(barrier, inc=1, device_id=peer, device_id_type=MESH)
    pl.semaphore_wait(barrier, len(peers))

    live = []

    def send(src, dst, target):
        k = len(live)
        copy = pltpu.make_async_remote_copy(
            src_ref=src,
            dst_ref=dst,
            send_sem=send_sem.at[k],
            recv_sem=recv_sem.at[k],
            device_id=target,
            device_id_type=MESH,
        )
        copy.start()
        live.append(copy)
        return copy

    def place(slot, j):
        return kv_out.at[slot, core, z_at[j]]

    kv_z, q_z, code_z, shared = {}, {}, {}, []
    for j, lands in ((1, 2), (2, 1), (3, 3)):
        kv_z[lands] = send(kv_ref.at[z_at[j]], kv_out.at[0, core, z], z_dev[j])
    kv_out[0, core, z] = kv_ref[z]
    q_out[z] = q_ref[z]
    code_out[z] = code_ref[...]

    from_up, from_down, far, halo_up, halo_down = {}, {}, {}, {}, {}

    def spread_own(j, src):
        from_down[j] = send(src, place(2, j), up)
        from_up[j] = send(src, place(1, j), down)
        if j == DIRECT:
            from_down["x"] = send(src, transit, back)
        shared.append(send(src, place(0, j), partner))

    def pass_on(j):
        from_up[j].wait_recv()
        if j in DOWN_SET:
            far[j] = send(place(1, j), place(3, j), down)
        if j != DIRECT:
            halo_up[j] = send(place(1, j), place(4, j), halo)
        shared.append(send(place(1, j), place(1, j), partner))
        from_down[j].wait_recv()
        if j in UP_SET:
            far[j] = send(place(2, j), place(3, j), up)
        if j != DIRECT:
            halo_down[j] = send(place(2, j), place(5, j), halo)
        shared.append(send(place(2, j), place(2, j), partner))

    spread_own(0, kv_ref.at[z])
    for j, lands in ((1, 2), (2, 1), (3, 3)):
        q_z[lands] = send(q_ref.at[z_at[j]], q_out.at[z], z_dev[j])
        code_z[lands] = send(code_ref, code_out.at[z], z_dev[j])
    for j in (1, 2):
        kv_z[j].wait_recv()
        spread_own(j, place(0, j))
    pass_on(0)
    kv_z[3].wait_recv()
    spread_own(3, place(0, 3))
    pass_on(1)
    pass_on(2)
    from_down["x"].wait_recv()
    halo_down[DIRECT] = send(transit, place(5, DIRECT), up)
    halo_up[DIRECT] = send(transit, place(4, DIRECT), down)
    pass_on(3)
    for j in range(4):
        far[j].wait_recv()
        shared.append(send(place(3, j), place(3, j), partner))
        halo_up[j].wait_recv()
        shared.append(send(place(4, j), place(4, j), partner))
        halo_down[j].wait_recv()
        shared.append(send(place(5, j), place(5, j), partner))
    for c in shared + list(q_z.values()) + list(code_z.values()):
        c.wait_recv()
    for c in live:
        c.wait_send()


COPIES = 3 + 6 + 2 * 4 + 1 + 4 + 4 + 6 + 2 + 8 + 12


def exchange(code, q, kv):
    tiles = kv.shape[1]
    piece = kv.shape[1:]
    return pl.pallas_call(
        exchange_kernel,
        out_shape=(
            jax.ShapeDtypeStruct((ZD,) + code.shape, jnp.int32),
            jax.ShapeDtypeStruct(q.shape, q.dtype),
            jax.ShapeDtypeStruct((6, 2, ZD) + piece, kv.dtype),
        ),
        in_specs=[pl.BlockSpec(memory_space=pltpu.VMEM)] * 3,
        out_specs=[pl.BlockSpec(memory_space=pltpu.VMEM)] * 3,
        scratch_shapes=[
            pltpu.VMEM(piece, kv.dtype),
            pltpu.SemaphoreType.DMA((COPIES,)),
            pltpu.SemaphoreType.DMA((COPIES,)),
        ],
        compiler_params=pltpu.CompilerParams(
            collective_id=0, has_side_effects=True, vmem_limit_bytes=24 * 1024 * 1024
        ),
    )(code, q, kv)


def attn_kernel(code_ref, q_ref, kv_ref, o_ref, s_ref):
    lane = lax.broadcasted_iota(jnp.int32, (1, TILE), 1)

    def one_tile(i, carry):
        groups = code_ref[i, NB] // 8
        q = q_ref[i]

        def scores(c, top):
            for p in range(4):
                a = code_ref[i, c * 8 + 2 * p]
                b = code_ref[i, c * 8 + 2 * p + 1]
                keys = jnp.concatenate([kv_ref[a // 256, 0], kv_ref[b // 256, 0]], axis=1)
                s = jnp.dot(q, keys, preferred_element_type=jnp.float32)
                bias = jnp.concatenate(
                    [
                        jnp.where(lane < a % 256, 0.0, NEG),
                        jnp.where(lane < b % 256, 0.0, NEG),
                    ],
                    axis=1,
                )
                s = s + bias
                s_ref[c, :, p * 256:(p + 1) * 256] = s
                top = jnp.maximum(top, jnp.maximum(s[:, :TILE], s[:, TILE:]))
            return top

        top = lax.fori_loop(0, groups, scores, jnp.full((TILE, TILE), NEG, jnp.float32))
        peak = jnp.max(top, axis=1, keepdims=True)

        def values(c, state):
            den, acc = state
            ps, vs = [], []
            for p in range(4):
                a = code_ref[i, c * 8 + 2 * p]
                b = code_ref[i, c * 8 + 2 * p + 1]
                w = jnp.exp2((s_ref[c, :, p * 256:(p + 1) * 256] - peak) * EXP_SCALE)
                den = den + (w[:, :TILE] + w[:, TILE:])
                ps.append(w.astype(jnp.bfloat16))
                vs += [kv_ref[a // 256, 1], kv_ref[b // 256, 1]]
            acc = acc + jnp.dot(
                jnp.concatenate(ps, axis=1),
                jnp.concatenate(vs, axis=0),
                preferred_element_type=jnp.float32,
            )
            return den, acc

        zero = jnp.zeros((TILE, TILE), jnp.float32)
        den, acc = lax.fori_loop(0, groups, values, (zero, zero))
        o_ref[i] = (acc / jnp.sum(den, axis=1, keepdims=True)).astype(jnp.bfloat16)
        return carry

    lax.fori_loop(0, q_ref.shape[0], one_tile, 0)


def attend(code, q, kv):
    return pl.pallas_call(
        attn_kernel,
        out_shape=jax.ShapeDtypeStruct(q.shape, jnp.bfloat16),
        in_specs=[
            pl.BlockSpec(memory_space=pltpu.SMEM),
            pl.BlockSpec(memory_space=pltpu.VMEM),
            pl.BlockSpec(memory_space=pltpu.VMEM),
        ],
        out_specs=pl.BlockSpec(memory_space=pltpu.VMEM),
        scratch_shapes=[pltpu.VMEM((4, TILE, 8 * TILE), jnp.float32)],
        compiler_params=pltpu.CompilerParams(vmem_limit_bytes=24 * 1024 * 1024),
    )(code, q, kv)


def finish_layer(node_features, attended, w_out, w_gate, w_up, w_down):
    residual = node_features.astype(jnp.float32) + jnp.dot(
        attended, w_out, preferred_element_type=jnp.float32
    )
    inverse = lax.rsqrt(jnp.mean(residual * residual, axis=-1, keepdims=True) + 1e-06)
    normed = (residual * inverse).astype(jnp.bfloat16)
    gate_part = jnp.dot(normed, w_gate, preferred_element_type=jnp.float32)
    up_part = jnp.dot(normed, w_up, preferred_element_type=jnp.float32)
    hidden = (jax.nn.silu(gate_part) * up_part).astype(jnp.bfloat16)
    return (residual + jnp.dot(hidden, w_down, preferred_element_type=jnp.float32)).astype(
        jnp.bfloat16
    )


def make_codes(neighbour_blocks, neighbour_count, tile_valid, zone_blocks, zone_count):
    zone = lax.axis_index("zone")
    y_lo = zone % 2
    y = (lax.axis_index("dev") // 8) * 2 + y_lo
    relative = (neighbour_blocks // zone_blocks - zone + 1) % zone_count
    local = neighbour_blocks % zone_blocks
    y_hi, rest = local // 32, local % 32
    z, rest = rest // 8, rest % 8
    core, t = rest // 4, rest % 4
    other_y = y_hi * 2 + 1 - y_lo
    above = (other_y - y + 4) % 4 == 1
    same_x = relative == 2 - 2 * y_lo
    near = jnp.where(same_x, jnp.where(above, 1, 2), jnp.where(above, 4, 5))
    slot = jnp.where(relative == 1, jnp.where(y_hi == y // 2, 0, 3), near)
    place = ((slot * 2 + core) * ZD + z) * 4 + t
    matches = neighbour_blocks[..., None] == jnp.arange(tile_valid.shape[0], dtype=jnp.int32)
    valid = jnp.sum(jnp.where(matches, tile_valid, 0), axis=-1)
    live = jnp.arange(NB, dtype=jnp.int32)[None, :] < neighbour_count[:, None]
    code = place * 256 + jnp.where(live, valid, 0)
    code = jnp.concatenate(
        [code, neighbour_count[:, None], jnp.zeros((code.shape[0], 95), jnp.int32)], axis=1
    )
    return jnp.concatenate([code, jnp.zeros_like(code)], axis=0)


def body(
    x,
    neighbour_blocks,
    neighbour_count,
    tile_valid,
    w_query,
    w_key,
    w_value,
    w_out,
    w_gate,
    w_up,
    w_down,
):
    rows = x.shape[0]
    tiles = rows // TILE
    zone_count = lax.axis_size("zone")
    dev_count = lax.axis_size("dev")
    z_groups = [
        [y * 8 + z * 2 + c for z in range(ZD)] for y in range(2) for c in range(2)
    ]
    codes = make_codes(
        neighbour_blocks, neighbour_count, tile_valid, tiles * dev_count, zone_count
    )
    q, kv = project(x, w_query, w_key, w_value)
    codes, q, kv = exchange(codes, q, kv)
    o = attend(
        codes[:, :tiles].reshape(ZD * tiles, -1),
        q.reshape(ZD * tiles, TILE, HD),
        kv.reshape(6 * 2 * ZD * tiles, 2, TILE, HD),
    )
    o = lax.all_to_all(
        o.reshape(ZD, tiles, TILE, HD), "dev", 0, 0, axis_index_groups=z_groups, tiled=True
    )
    attended = jnp.transpose(o, (1, 2, 0, 3)).reshape(rows, D)
    return finish_layer(x, attended, w_out, w_gate, w_up, w_down)


def solution(mesh):
    placed = (
        P(("zone", "dev"), None),
        P(("zone", "dev"), None),
        P(("zone", "dev")),
        P(),
        P(),
        P(),
        P(),
        P(),
        P(),
        P(),
        P(),
    )
    return jax.shard_map(
        body, mesh=mesh, in_specs=placed, out_specs=P(("zone", "dev"), None), check_vma=False
    )
```

```python
import functools
import math

import jax
import jax.numpy as jnp
from jax import lax
from jax.experimental import pallas as pl
from jax.experimental.pallas import tpu as pltpu
from jax.sharding import PartitionSpec as P

D = 512
HEADS = 4
HD = 128
TILE = 128
NB = 32
ZD = 4
NEG = -1e30
EXP_SCALE = math.log2(math.e) / math.sqrt(HD)


def proj_kernel(x_ref, wq_ref, wk_ref, wv_ref, q_ref, kv_ref):
    def one_tile(t, carry):
        x = x_ref[pl.ds(pl.multiple_of(t * TILE, TILE), TILE), :]
        q = jnp.dot(x, wq_ref[...], preferred_element_type=jnp.float32).astype(jnp.bfloat16)
        for h in range(HEADS):
            q_ref[h, t] = q[:, h * HD:(h + 1) * HD]
        k = jnp.dot(x, wk_ref[...], preferred_element_type=jnp.float32)
        for h in range(HEADS):
            kv_ref[h, t, 0] = jnp.transpose(k[:, h * HD:(h + 1) * HD]).astype(jnp.bfloat16)
        v = jnp.dot(x, wv_ref[...], preferred_element_type=jnp.float32).astype(jnp.bfloat16)
        for h in range(HEADS):
            kv_ref[h, t, 1] = v[:, h * HD:(h + 1) * HD]
        return carry

    lax.fori_loop(0, x_ref.shape[0] // TILE, one_tile, 0)


def project(x, wq, wk, wv):
    tiles = x.shape[0] // TILE
    return pl.pallas_call(
        proj_kernel,
        out_shape=(
            jax.ShapeDtypeStruct((HEADS, tiles, TILE, HD), jnp.bfloat16),
            jax.ShapeDtypeStruct((HEADS, tiles, 2, TILE, HD), jnp.bfloat16),
        ),
    )(x, wq, wk, wv)


MESH = pl.DeviceIdType.MESH
DIRECT = 3
UP_SET = (0, 2)
DOWN_SET = (1, 3)


def exchange_kernel(code_ref, q_ref, kv_ref, code_out, q_out, kv_out, transit, send_sem, recv_sem):
    zone, dev = lax.axis_index("zone"), lax.axis_index("dev")
    x, y_lo = zone // 2, zone % 2
    y_hi, z, core = dev // 8, (dev // 2) % ZD, dev % 2
    y = y_hi * 2 + y_lo

    def at(px, py, pz, pc):
        return (px * 2 + py % 2, (py // 2) * 8 + pz * 2 + pc)

    side = 1 - 2 * y_lo
    up, down = at(x, (y + 1) % 4, z, core), at(x, (y + 3) % 4, z, core)
    halo, back = at((x + 4 + side) % 4, y, z, core), at((x + 4 - side) % 4, y, z, core)
    partner = at(x, y, z, 1 - core)
    z_at = [z] + [(z + d) % ZD for d in (1, 3, 2)]
    z_dev = [None] + [at(x, y, z_at[j], core) for j in (1, 2, 3)]

    barrier = pltpu.get_barrier_semaphore()
    peers = [up, down, halo, back, partner] + z_dev[1:]
    for peer in peers:
        pl.semaphore_signal(barrier, inc=1, device_id=peer, device_id_type=MESH)
    pl.semaphore_wait(barrier, len(peers))

    live = []

    def send(src, dst, target):
        k = len(live)
        copy = pltpu.make_async_remote_copy(
            src_ref=src,
            dst_ref=dst,
            send_sem=send_sem.at[k],
            recv_sem=recv_sem.at[k],
            device_id=target,
            device_id_type=MESH,
        )
        copy.start()
        live.append(copy)
        return copy

    def place(slot, j):
        return kv_out.at[slot, core, z_at[j]]

    kv_z, q_z, code_z, shared = {}, {}, {}, []
    for j, lands in ((1, 2), (2, 1), (3, 3)):
        kv_z[lands] = send(kv_ref.at[z_at[j]], kv_out.at[0, core, z], z_dev[j])
    kv_out[0, core, z] = kv_ref[z]
    q_out[z] = q_ref[z]
    code_out[z] = code_ref[...]

    from_up, from_down, far, halo_up, halo_down = {}, {}, {}, {}, {}

    def spread_own(j, src):
        from_down[j] = send(src, place(2, j), up)
        from_up[j] = send(src, place(1, j), down)
        if j == DIRECT:
            from_down["x"] = send(src, transit, back)
        shared.append(send(src, place(0, j), partner))

    def pass_on(j):
        from_up[j].wait_recv()
        if j in DOWN_SET:
            far[j] = send(place(1, j), place(3, j), down)
        if j != DIRECT:
            halo_up[j] = send(place(1, j), place(4, j), halo)
        shared.append(send(place(1, j), place(1, j), partner))
        from_down[j].wait_recv()
        if j in UP_SET:
            far[j] = send(place(2, j), place(3, j), up)
        if j != DIRECT:
            halo_down[j] = send(place(2, j), place(5, j), halo)
        shared.append(send(place(2, j), place(2, j), partner))

    spread_own(0, kv_ref.at[z])
    for j, lands in ((1, 2), (2, 1), (3, 3)):
        q_z[lands] = send(q_ref.at[z_at[j]], q_out.at[z], z_dev[j])
        code_z[lands] = send(code_ref, code_out.at[z], z_dev[j])
    for j in (1, 2):
        kv_z[j].wait_recv()
        spread_own(j, place(0, j))
    pass_on(0)
    kv_z[3].wait_recv()
    spread_own(3, place(0, 3))
    pass_on(1)
    pass_on(2)
    from_down["x"].wait_recv()
    halo_down[DIRECT] = send(transit, place(5, DIRECT), up)
    halo_up[DIRECT] = send(transit, place(4, DIRECT), down)
    pass_on(3)
    for j in range(4):
        far[j].wait_recv()
        shared.append(send(place(3, j), place(3, j), partner))
        halo_up[j].wait_recv()
        shared.append(send(place(4, j), place(4, j), partner))
        halo_down[j].wait_recv()
        shared.append(send(place(5, j), place(5, j), partner))
    for c in shared + list(q_z.values()) + list(code_z.values()):
        c.wait_recv()
    for c in live:
        c.wait_send()


COPIES = 3 + 6 + 2 * 4 + 1 + 4 + 4 + 6 + 2 + 8 + 12


def exchange(code, q, kv):
    tiles = kv.shape[1]
    piece = kv.shape[1:]
    return pl.pallas_call(
        exchange_kernel,
        out_shape=(
            jax.ShapeDtypeStruct((ZD,) + code.shape, jnp.int32),
            jax.ShapeDtypeStruct(q.shape, q.dtype),
            jax.ShapeDtypeStruct((6, 2, ZD) + piece, kv.dtype),
        ),
        in_specs=[pl.BlockSpec(memory_space=pltpu.VMEM)] * 3,
        out_specs=[pl.BlockSpec(memory_space=pltpu.VMEM)] * 3,
        scratch_shapes=[
            pltpu.VMEM(piece, kv.dtype),
            pltpu.SemaphoreType.DMA((COPIES,)),
            pltpu.SemaphoreType.DMA((COPIES,)),
        ],
        compiler_params=pltpu.CompilerParams(
            collective_id=0, has_side_effects=True, vmem_limit_bytes=24 * 1024 * 1024
        ),
    )(code, q, kv)


LEAD = 5


def attn_kernel(code_ref, q_ref, kv_ref, o_ref, s_even, s_odd, top_ref, den_ref, acc_ref):
    tiles = q_ref.shape[0]
    lane = lax.broadcasted_iota(jnp.int32, (1, TILE), 1)
    rings = (s_even, s_odd)

    def groups(i):
        return code_ref[i, NB] // 8

    def advance(i, c):
        last = c + 1 >= groups(i)
        return jnp.where(last, jnp.minimum(i + 1, tiles), i), jnp.where(last, 0, c + 1)

    def scores(i, c, ring, slot):
        q = q_ref[jnp.minimum(i, tiles - 1)]
        top = jnp.where(c == 0, NEG, top_ref[i])
        for p in range(4):
            a = code_ref[i, c * 8 + 2 * p]
            b = code_ref[i, c * 8 + 2 * p + 1]
            keys = jnp.concatenate([kv_ref[a // 256, 0], kv_ref[b // 256, 0]], axis=1)
            s = jnp.dot(q, keys, preferred_element_type=jnp.float32)
            bias = jnp.concatenate(
                [jnp.where(lane < a % 256, 0.0, NEG), jnp.where(lane < b % 256, 0.0, NEG)],
                axis=1,
            )
            s = s + bias
            ring[slot, :, p * 256:(p + 1) * 256] = s
            top = jnp.maximum(top, jnp.maximum(s[:, :TILE], s[:, TILE:]))
        top_ref[i] = top

    def values(i, c, peak, ring, slot):
        den = jnp.where(c == 0, 0.0, den_ref[...])
        acc = jnp.where(c == 0, 0.0, acc_ref[...])
        ps, vs = [], []
        for p in range(4):
            a = code_ref[i, c * 8 + 2 * p]
            b = code_ref[i, c * 8 + 2 * p + 1]
            w = jnp.exp2((ring[slot, :, p * 256:(p + 1) * 256] - peak) * EXP_SCALE)
            den = den + (w[:, :TILE] + w[:, TILE:])
            ps.append(w.astype(jnp.bfloat16))
            vs += [kv_ref[a // 256, 1], kv_ref[b // 256, 1]]
        acc = acc + jnp.dot(
            jnp.concatenate(ps, axis=1),
            jnp.concatenate(vs, axis=0),
            preferred_element_type=jnp.float32,
        )
        den_ref[...] = den
        acc_ref[...] = acc
        o_ref[i] = (acc / jnp.sum(den, axis=1, keepdims=True)).astype(jnp.bfloat16)

    total = lax.fori_loop(0, tiles, lambda i, n: n + groups(i), 0)
    head = (jnp.int32(0), jnp.int32(0))
    for w in range(LEAD):
        scores(*head, rings[w % 2], w // 2)
        head = advance(*head)

    def pair(k, state):
        head, tail = state
        tails = (tail, advance(*tail))
        peaks = [jnp.max(top_ref[i], axis=1, keepdims=True) for i, _ in tails]
        for r in range(2):
            w = 2 * k + r
            scores(*head, rings[(r + LEAD) % 2], ((w + LEAD) // 2) % 4)
            values(*tails[r], peaks[r], rings[r], (w // 2) % 4)
            head = advance(*head)
        return head, advance(*tails[1])

    lax.fori_loop(0, (total + 1) // 2, pair, (head, (jnp.int32(0), jnp.int32(0))))


def attend(code, q, kv):
    tiles = q.shape[0]
    ring = pltpu.VMEM((4, TILE, 8 * TILE), jnp.float32)
    square = pltpu.VMEM((TILE, TILE), jnp.float32)
    return pl.pallas_call(
        attn_kernel,
        out_shape=jax.ShapeDtypeStruct((tiles + 1,) + q.shape[1:], jnp.bfloat16),
        in_specs=[
            pl.BlockSpec(memory_space=pltpu.SMEM),
            pl.BlockSpec(memory_space=pltpu.VMEM),
            pl.BlockSpec(memory_space=pltpu.VMEM),
        ],
        out_specs=pl.BlockSpec(memory_space=pltpu.VMEM),
        scratch_shapes=[
            ring, ring, pltpu.VMEM((tiles + 1, TILE, TILE), jnp.float32), square, square
        ],
        compiler_params=pltpu.CompilerParams(vmem_limit_bytes=24 * 1024 * 1024),
    )(code, q, kv)


def finish_layer(node_features, attended, w_out, w_gate, w_up, w_down):
    residual = node_features.astype(jnp.float32) + jnp.dot(
        attended, w_out, preferred_element_type=jnp.float32
    )
    inverse = lax.rsqrt(jnp.mean(residual * residual, axis=-1, keepdims=True) + 1e-06)
    normed = (residual * inverse).astype(jnp.bfloat16)
    gate_part = jnp.dot(normed, w_gate, preferred_element_type=jnp.float32)
    up_part = jnp.dot(normed, w_up, preferred_element_type=jnp.float32)
    hidden = (jax.nn.silu(gate_part) * up_part).astype(jnp.bfloat16)
    return (residual + jnp.dot(hidden, w_down, preferred_element_type=jnp.float32)).astype(
        jnp.bfloat16
    )


def make_codes(neighbour_blocks, neighbour_count, tile_valid, zone_blocks, zone_count):
    zone = lax.axis_index("zone")
    y_lo = zone % 2
    y = (lax.axis_index("dev") // 8) * 2 + y_lo
    relative = (neighbour_blocks // zone_blocks - zone + 1) % zone_count
    local = neighbour_blocks % zone_blocks
    y_hi, rest = local // 32, local % 32
    z, rest = rest // 8, rest % 8
    core, t = rest // 4, rest % 4
    other_y = y_hi * 2 + 1 - y_lo
    above = (other_y - y + 4) % 4 == 1
    same_x = relative == 2 - 2 * y_lo
    near = jnp.where(same_x, jnp.where(above, 1, 2), jnp.where(above, 4, 5))
    slot = jnp.where(relative == 1, jnp.where(y_hi == y // 2, 0, 3), near)
    place = ((slot * 2 + core) * ZD + z) * 4 + t
    matches = neighbour_blocks[..., None] == jnp.arange(tile_valid.shape[0], dtype=jnp.int32)
    valid = jnp.sum(jnp.where(matches, tile_valid, 0), axis=-1)
    live = jnp.arange(NB, dtype=jnp.int32)[None, :] < neighbour_count[:, None]
    code = place * 256 + jnp.where(live, valid, 0)
    code = jnp.concatenate(
        [code, neighbour_count[:, None], jnp.zeros((code.shape[0], 95), jnp.int32)], axis=1
    )
    return jnp.concatenate([code, jnp.zeros_like(code)], axis=0)


def body(
    x,
    neighbour_blocks,
    neighbour_count,
    tile_valid,
    w_query,
    w_key,
    w_value,
    w_out,
    w_gate,
    w_up,
    w_down,
):
    rows = x.shape[0]
    tiles = rows // TILE
    zone_count = lax.axis_size("zone")
    dev_count = lax.axis_size("dev")
    z_groups = [
        [y * 8 + z * 2 + c for z in range(ZD)] for y in range(2) for c in range(2)
    ]
    codes = make_codes(
        neighbour_blocks, neighbour_count, tile_valid, tiles * dev_count, zone_count
    )
    q, kv = project(x, w_query, w_key, w_value)
    codes, q, kv = exchange(codes, q, kv)
    o = attend(
        jnp.pad(codes[:, :tiles].reshape(ZD * tiles, -1), ((0, 8), (0, 0))),
        q.reshape(ZD * tiles, TILE, HD),
        kv.reshape(6 * 2 * ZD * tiles, 2, TILE, HD),
    )
    o = lax.all_to_all(
        o[:ZD * tiles].reshape(ZD, tiles, TILE, HD), "dev", 0, 0, axis_index_groups=z_groups, tiled=True
    )
    attended = jnp.transpose(o, (1, 2, 0, 3)).reshape(rows, D)
    return finish_layer(x, attended, w_out, w_gate, w_up, w_down)


def solution(mesh):
    placed = (
        P(("zone", "dev"), None),
        P(("zone", "dev"), None),
        P(("zone", "dev")),
        P(),
        P(),
        P(),
        P(),
        P(),
        P(),
        P(),
        P(),
    )
    return jax.shard_map(
        body, mesh=mesh, in_specs=placed, out_specs=P(("zone", "dev"), None), check_vma=False
    )
```

```python
import functools
import math

import jax
import jax.numpy as jnp
from jax import lax
from jax.experimental import pallas as pl
from jax.experimental.pallas import tpu as pltpu
from jax.sharding import PartitionSpec as P

D = 512
HEADS = 4
HD = 128
TILE = 128
NB = 32
ZD = 4
NEG = -1e30
EXP_SCALE = math.log2(math.e) / math.sqrt(HD)


def proj_kernel(x_ref, wq_ref, wk_ref, wv_ref, q_ref, kv_ref):
    def one_tile(t, carry):
        x = x_ref[pl.ds(pl.multiple_of(t * TILE, TILE), TILE), :]
        q = jnp.dot(x, wq_ref[...], preferred_element_type=jnp.float32).astype(jnp.bfloat16)
        for h in range(HEADS):
            q_ref[h, t] = q[:, h * HD:(h + 1) * HD]
        k = jnp.dot(x, wk_ref[...], preferred_element_type=jnp.float32)
        for h in range(HEADS):
            kv_ref[h, t, 0] = jnp.transpose(k[:, h * HD:(h + 1) * HD]).astype(jnp.bfloat16)
        v = jnp.dot(x, wv_ref[...], preferred_element_type=jnp.float32).astype(jnp.bfloat16)
        for h in range(HEADS):
            kv_ref[h, t, 1] = v[:, h * HD:(h + 1) * HD]
        return carry

    lax.fori_loop(0, x_ref.shape[0] // TILE, one_tile, 0)


def project(x, wq, wk, wv):
    tiles = x.shape[0] // TILE
    return pl.pallas_call(
        proj_kernel,
        out_shape=(
            jax.ShapeDtypeStruct((HEADS, tiles, TILE, HD), jnp.bfloat16),
            jax.ShapeDtypeStruct((HEADS, tiles, 2, TILE, HD), jnp.bfloat16),
        ),
    )(x, wq, wk, wv)


MESH = pl.DeviceIdType.MESH
DIRECT = 3
UP_SET = (0, 2)
DOWN_SET = (1, 3)


def exchange_kernel(code_ref, q_ref, kv_ref, code_out, q_out, kv_out, transit, send_sem, recv_sem):
    zone, dev = lax.axis_index("zone"), lax.axis_index("dev")
    x, y_lo = zone // 2, zone % 2
    y_hi, z, core = dev // 8, (dev // 2) % ZD, dev % 2
    y = y_hi * 2 + y_lo

    def at(px, py, pz, pc):
        return (px * 2 + py % 2, (py // 2) * 8 + pz * 2 + pc)

    side = 1 - 2 * y_lo
    up, down = at(x, (y + 1) % 4, z, core), at(x, (y + 3) % 4, z, core)
    halo, back = at((x + 4 + side) % 4, y, z, core), at((x + 4 - side) % 4, y, z, core)
    partner = at(x, y, z, 1 - core)
    z_at = [z] + [(z + d) % ZD for d in (1, 3, 2)]
    z_dev = [None] + [at(x, y, z_at[j], core) for j in (1, 2, 3)]

    barrier = pltpu.get_barrier_semaphore()
    peers = [up, down, halo, back, partner] + z_dev[1:]
    for peer in peers:
        pl.semaphore_signal(barrier, inc=1, device_id=peer, device_id_type=MESH)
    pl.semaphore_wait(barrier, len(peers))

    live = []

    def send(src, dst, target):
        k = len(live)
        copy = pltpu.make_async_remote_copy(
            src_ref=src,
            dst_ref=dst,
            send_sem=send_sem.at[k],
            recv_sem=recv_sem.at[k],
            device_id=target,
            device_id_type=MESH,
        )
        copy.start()
        live.append(copy)
        return copy

    def place(slot, j):
        return kv_out.at[slot, core, z_at[j]]

    kv_z, q_z, code_z, shared = {}, {}, {}, []
    for j, lands in ((1, 2), (2, 1), (3, 3)):
        kv_z[lands] = send(kv_ref.at[z_at[j]], kv_out.at[0, core, z], z_dev[j])
    kv_out[0, core, z] = kv_ref[z]
    q_out[z] = q_ref[z]
    code_out[z] = code_ref[...]

    from_up, from_down, far, halo_up, halo_down = {}, {}, {}, {}, {}

    def spread_own(j, src):
        from_down[j] = send(src, place(2, j), up)
        from_up[j] = send(src, place(1, j), down)
        if j == DIRECT:
            from_down["x"] = send(src, transit, back)
        shared.append(send(src, place(0, j), partner))

    def pass_on(j):
        from_up[j].wait_recv()
        if j in DOWN_SET:
            far[j] = send(place(1, j), place(3, j), down)
        if j != DIRECT:
            halo_up[j] = send(place(1, j), place(4, j), halo)
        shared.append(send(place(1, j), place(1, j), partner))
        from_down[j].wait_recv()
        if j in UP_SET:
            far[j] = send(place(2, j), place(3, j), up)
        if j != DIRECT:
            halo_down[j] = send(place(2, j), place(5, j), halo)
        shared.append(send(place(2, j), place(2, j), partner))

    spread_own(0, kv_ref.at[z])
    for j, lands in ((1, 2), (2, 1), (3, 3)):
        q_z[lands] = send(q_ref.at[z_at[j]], q_out.at[z], z_dev[j])
        code_z[lands] = send(code_ref, code_out.at[z], z_dev[j])
    for j in (1, 2):
        kv_z[j].wait_recv()
        spread_own(j, place(0, j))
    pass_on(0)
    kv_z[3].wait_recv()
    spread_own(3, place(0, 3))
    pass_on(1)
    pass_on(2)
    from_down["x"].wait_recv()
    halo_down[DIRECT] = send(transit, place(5, DIRECT), up)
    halo_up[DIRECT] = send(transit, place(4, DIRECT), down)
    pass_on(3)
    for j in range(4):
        far[j].wait_recv()
        shared.append(send(place(3, j), place(3, j), partner))
        halo_up[j].wait_recv()
        shared.append(send(place(4, j), place(4, j), partner))
        halo_down[j].wait_recv()
        shared.append(send(place(5, j), place(5, j), partner))
    for c in shared + list(q_z.values()) + list(code_z.values()):
        c.wait_recv()
    for c in live:
        c.wait_send()


COPIES = 3 + 6 + 2 * 4 + 1 + 4 + 4 + 6 + 2 + 8 + 12


def exchange(code, q, kv):
    tiles = kv.shape[1]
    piece = kv.shape[1:]
    return pl.pallas_call(
        exchange_kernel,
        out_shape=(
            jax.ShapeDtypeStruct((ZD,) + code.shape, jnp.int32),
            jax.ShapeDtypeStruct(q.shape, q.dtype),
            jax.ShapeDtypeStruct((6, 2, ZD) + piece, kv.dtype),
        ),
        in_specs=[pl.BlockSpec(memory_space=pltpu.VMEM)] * 3,
        out_specs=[pl.BlockSpec(memory_space=pltpu.VMEM)] * 3,
        scratch_shapes=[
            pltpu.VMEM(piece, kv.dtype),
            pltpu.SemaphoreType.DMA((COPIES,)),
            pltpu.SemaphoreType.DMA((COPIES,)),
        ],
        compiler_params=pltpu.CompilerParams(
            collective_id=0, has_side_effects=True, vmem_limit_bytes=24 * 1024 * 1024
        ),
    )(code, q, kv)


LEAD = 5


def attn_kernel(code_ref, q_ref, kv_ref, o_ref, s_even, s_odd, top_ref, den_ref, acc_ref):
    tiles = q_ref.shape[0]
    lane = lax.broadcasted_iota(jnp.int32, (1, TILE), 1)
    rings = (s_even, s_odd)

    def groups(i):
        return code_ref[i, NB] // 8

    def advance(i, c):
        last = c + 1 >= groups(i)
        return jnp.where(last, jnp.minimum(i + 1, tiles), i), jnp.where(last, 0, c + 1)

    def scores(i, c, ring, slot):
        q = q_ref[jnp.minimum(i, tiles - 1)]
        top = jnp.where(c == 0, NEG, top_ref[i])
        for p in range(4):
            a = code_ref[i, c * 8 + 2 * p]
            b = code_ref[i, c * 8 + 2 * p + 1]
            keys = jnp.concatenate([kv_ref[a // 256, 0], kv_ref[b // 256, 0]], axis=1)
            s = jnp.dot(q, keys, preferred_element_type=jnp.float32)
            bias = jnp.concatenate(
                [jnp.where(lane < a % 256, 0.0, NEG), jnp.where(lane < b % 256, 0.0, NEG)],
                axis=1,
            )
            s = s + bias
            ring[slot, :, p * 256:(p + 1) * 256] = s
            top = jnp.maximum(top, jnp.maximum(s[:, :TILE], s[:, TILE:]))
        top_ref[i] = top

    def values(i, c, peak, ring, slot):
        den = jnp.where(c == 0, 0.0, den_ref[...])
        acc = jnp.where(c == 0, 0.0, acc_ref[...])
        ps, vs = [], []
        for p in range(4):
            a = code_ref[i, c * 8 + 2 * p]
            b = code_ref[i, c * 8 + 2 * p + 1]
            w = jnp.exp2((ring[slot, :, p * 256:(p + 1) * 256] - peak) * EXP_SCALE)
            den = den + (w[:, :TILE] + w[:, TILE:])
            ps.append(w.astype(jnp.bfloat16))
            vs += [kv_ref[a // 256, 1], kv_ref[b // 256, 1]]
        acc = acc + jnp.dot(
            jnp.concatenate(ps, axis=1),
            jnp.concatenate(vs, axis=0),
            preferred_element_type=jnp.float32,
        )
        den_ref[...] = den
        acc_ref[...] = acc
        o_ref[i] = (acc / jnp.sum(den, axis=1, keepdims=True)).astype(jnp.bfloat16)

    total = lax.fori_loop(0, tiles, lambda i, n: n + groups(i), 0)
    head = (jnp.int32(0), jnp.int32(0))
    for w in range(LEAD):
        scores(*head, rings[w % 2], w // 2)
        head = advance(*head)

    def pair(k, state):
        head, tail = state
        tails = (tail, advance(*tail))
        peaks = [jnp.max(top_ref[i], axis=1, keepdims=True) for i, _ in tails]
        for r in range(2):
            w = 2 * k + r
            scores(*head, rings[(r + LEAD) % 2], ((w + LEAD) // 2) % 4)
            values(*tails[r], peaks[r], rings[r], (w // 2) % 4)
            head = advance(*head)
        return head, advance(*tails[1])

    lax.fori_loop(0, (total + 1) // 2, pair, (head, (jnp.int32(0), jnp.int32(0))))


def attend(code, q, kv):
    tiles = q.shape[0]
    ring = pltpu.VMEM((4, TILE, 8 * TILE), jnp.float32)
    square = pltpu.VMEM((TILE, TILE), jnp.float32)
    return pl.pallas_call(
        attn_kernel,
        out_shape=jax.ShapeDtypeStruct((tiles + 1,) + q.shape[1:], jnp.bfloat16),
        in_specs=[
            pl.BlockSpec(memory_space=pltpu.SMEM),
            pl.BlockSpec(memory_space=pltpu.VMEM),
            pl.BlockSpec(memory_space=pltpu.VMEM),
        ],
        out_specs=pl.BlockSpec(memory_space=pltpu.VMEM),
        scratch_shapes=[
            ring, ring, pltpu.VMEM((tiles + 1, TILE, TILE), jnp.float32), square, square
        ],
        compiler_params=pltpu.CompilerParams(vmem_limit_bytes=24 * 1024 * 1024),
    )(code, q, kv)


def finish_kernel(
    o_ref, x_hbm, wo_hbm, wg_hbm, wu_hbm, wd_hbm, out_ref,
    x_ref, wo_ref, wg_ref, wu_ref, wd_ref, got, res_ref, norm_ref, hid_ref,
    load_sem, send_sem, recv_sem,
):
    dev = lax.axis_index("dev")
    zone = lax.axis_index("zone")
    z = (dev // 2) % ZD
    tiles = x_ref.shape[0] // TILE
    z_at = [(z + d) % ZD for d in (1, 3, 2)]
    peers = [(zone, dev + 2 * (pz - z)) for pz in z_at]

    barrier = pltpu.get_barrier_semaphore()
    for peer in peers:
        pl.semaphore_signal(barrier, inc=1, device_id=peer, device_id_type=MESH)
    loads = [
        pltpu.make_async_copy(src, dst, load_sem.at[i])
        for i, (src, dst) in enumerate(
            (
                (x_hbm, x_ref), (wo_hbm, wo_ref), (wg_hbm, wg_ref), (wu_hbm, wu_ref), (wd_hbm, wd_ref)
            )
        )
    ]
    for c in loads:
        c.start()
    pl.semaphore_wait(barrier, len(peers))
    copies = {}
    for k, lands in ((2, 2), (0, 1), (1, 0)):
        copies[lands] = pltpu.make_async_remote_copy(
            src_ref=o_ref.at[pl.ds(z_at[k] * tiles, tiles)],
            dst_ref=got.at[lands],
            send_sem=send_sem.at[lands],
            recv_sem=recv_sem.at[lands],
            device_id=peers[k],
            device_id_type=MESH,
        )
        copies[lands].start()

    def add_head(head, piece):
        o = piece.reshape(tiles * TILE, HD)
        w = wo_ref[pl.ds(pl.multiple_of(head * HD, HD), HD), :]
        return jnp.dot(o, w, preferred_element_type=jnp.float32)

    loads[0].wait()
    loads[1].wait()
    res_ref[...] = x_ref[...].astype(jnp.float32) + add_head(
        z, o_ref[pl.ds(z * tiles, tiles)]
    )
    for k in (0, 1, 2):
        copies[k].wait_recv()
        res_ref[...] += add_head(z_at[k], got[k])
    r = res_ref[...]
    inverse = lax.rsqrt(jnp.mean(r * r, axis=-1, keepdims=True) + 1e-06)
    norm_ref[...] = (r * inverse).astype(jnp.bfloat16)
    loads[2].wait()
    loads[3].wait()
    width = 256

    def hidden(f, carry):
        cols = pl.ds(pl.multiple_of(f * width, width), width)
        gate = jnp.dot(norm_ref[...], wg_ref[:, cols], preferred_element_type=jnp.float32)
        up = jnp.dot(norm_ref[...], wu_ref[:, cols], preferred_element_type=jnp.float32)
        hid_ref[:, cols] = (gate / (1.0 + jnp.exp(-gate)) * up).astype(jnp.bfloat16)
        return carry

    lax.fori_loop(0, wg_ref.shape[1] // width, hidden, 0)
    loads[4].wait()

    def down(f, carry):
        cols = pl.ds(pl.multiple_of(f * width, width), width)
        out_ref[:, cols] = (
            res_ref[:, cols]
            + jnp.dot(hid_ref[...], wd_ref[:, cols], preferred_element_type=jnp.float32)
        ).astype(jnp.bfloat16)
        return carry

    lax.fori_loop(0, D // width, down, 0)
    for c in copies.values():
        c.wait_send()


def finish_layer(o, x, w_out, w_gate, w_up, w_down):
    rows = x.shape[0]
    tiles = rows // TILE
    ff = w_gate.shape[1]
    return pl.pallas_call(
        finish_kernel,
        out_shape=jax.ShapeDtypeStruct(x.shape, x.dtype),
        in_specs=[pl.BlockSpec(memory_space=pltpu.VMEM)]
        + [pl.BlockSpec(memory_space=pl.ANY)] * 5,
        out_specs=pl.BlockSpec(memory_space=pltpu.VMEM),
        scratch_shapes=[
            pltpu.VMEM(x.shape, x.dtype),
            pltpu.VMEM(w_out.shape, w_out.dtype),
            pltpu.VMEM(w_gate.shape, w_gate.dtype),
            pltpu.VMEM(w_up.shape, w_up.dtype),
            pltpu.VMEM(w_down.shape, w_down.dtype),
            pltpu.VMEM((ZD - 1, tiles, TILE, HD), jnp.bfloat16),
            pltpu.VMEM(x.shape, jnp.float32),
            pltpu.VMEM(x.shape, jnp.bfloat16),
            pltpu.VMEM((rows, ff), jnp.bfloat16),
            pltpu.SemaphoreType.DMA((5,)),
            pltpu.SemaphoreType.DMA((ZD - 1,)),
            pltpu.SemaphoreType.DMA((ZD - 1,)),
        ],
        compiler_params=pltpu.CompilerParams(
            collective_id=1, has_side_effects=True, vmem_limit_bytes=24 * 1024 * 1024
        ),
    )(o, x, w_out, w_gate, w_up, w_down)


def make_codes(neighbour_blocks, neighbour_count, tile_valid, zone_blocks, zone_count):
    zone = lax.axis_index("zone")
    y_lo = zone % 2
    y = (lax.axis_index("dev") // 8) * 2 + y_lo
    relative = (neighbour_blocks // zone_blocks - zone + 1) % zone_count
    local = neighbour_blocks % zone_blocks
    y_hi, rest = local // 32, local % 32
    z, rest = rest // 8, rest % 8
    core, t = rest // 4, rest % 4
    other_y = y_hi * 2 + 1 - y_lo
    above = (other_y - y + 4) % 4 == 1
    same_x = relative == 2 - 2 * y_lo
    near = jnp.where(same_x, jnp.where(above, 1, 2), jnp.where(above, 4, 5))
    slot = jnp.where(relative == 1, jnp.where(y_hi == y // 2, 0, 3), near)
    place = ((slot * 2 + core) * ZD + z) * 4 + t
    matches = neighbour_blocks[..., None] == jnp.arange(tile_valid.shape[0], dtype=jnp.int32)
    valid = jnp.sum(jnp.where(matches, tile_valid, 0), axis=-1)
    live = jnp.arange(NB, dtype=jnp.int32)[None, :] < neighbour_count[:, None]
    code = place * 256 + jnp.where(live, valid, 0)
    code = jnp.concatenate(
        [code, neighbour_count[:, None], jnp.zeros((code.shape[0], 95), jnp.int32)], axis=1
    )
    return jnp.concatenate([code, jnp.zeros_like(code)], axis=0)


def body(
    x,
    neighbour_blocks,
    neighbour_count,
    tile_valid,
    w_query,
    w_key,
    w_value,
    w_out,
    w_gate,
    w_up,
    w_down,
):
    rows = x.shape[0]
    tiles = rows // TILE
    zone_count = lax.axis_size("zone")
    dev_count = lax.axis_size("dev")
    codes = make_codes(
        neighbour_blocks, neighbour_count, tile_valid, tiles * dev_count, zone_count
    )
    q, kv = project(x, w_query, w_key, w_value)
    codes, q, kv = exchange(codes, q, kv)
    o = attend(
        jnp.pad(codes[:, :tiles].reshape(ZD * tiles, -1), ((0, 8), (0, 0))),
        q.reshape(ZD * tiles, TILE, HD),
        kv.reshape(6 * 2 * ZD * tiles, 2, TILE, HD),
    )
    return finish_layer(o, x, w_out, w_gate, w_up, w_down)


def solution(mesh):
    placed = (
        P(("zone", "dev"), None),
        P(("zone", "dev"), None),
        P(("zone", "dev")),
        P(),
        P(),
        P(),
        P(),
        P(),
        P(),
        P(),
        P(),
    )
    return jax.shard_map(
        body, mesh=mesh, in_specs=placed, out_specs=P(("zone", "dev"), None), check_vma=False
    )
```

```python
import math

import jax
import jax.numpy as jnp
from jax import lax
from jax.experimental import pallas as pl
from jax.experimental.pallas import tpu as pltpu
from jax.sharding import PartitionSpec as P

D = 512
HEADS = 4
HD = 128
TILE = 128
NB = 32
ZD = 4
NEG = -1e30
EXP_SCALE = math.log2(math.e) / math.sqrt(HD)


MESH = pl.DeviceIdType.MESH
UNITS = tuple((j, h) for j in range(ZD) for h in range(2))
DIRECT = ((1, 0), (1, 1), (2, 1))
COPIES = 112


def exchange_kernel(
    nb_ref, count_ref, valid_ref, x_ref, wq_ref, wk_ref, wv_ref,
    code_out, q_out, kv_out,
    kv_ref, q_ref, raw, raw_all, relay, transit, send_sem, recv_sem,
):
    zone, dev = lax.axis_index("zone"), lax.axis_index("dev")
    x, y_lo = zone // 2, zone % 2
    y_hi, z, core = dev // 8, (dev // 2) % ZD, dev % 2
    y = y_hi * 2 + y_lo
    tiles = x_ref.shape[0] // TILE
    half = tiles // 2

    def at(px, py, pz, pc):
        return (px * 2 + py % 2, (py // 2) * 8 + pz * 2 + pc)

    side = 1 - 2 * y_lo
    up, down = at(x, (y + 1) % 4, z, core), at(x, (y + 3) % 4, z, core)
    halo, back = at((x + 4 + side) % 4, y, z, core), at((x + 4 - side) % 4, y, z, core)
    partner = at(x, y, z, 1 - core)
    z_at = [(z + d) % ZD for d in (0, 1, 3, 2)]
    z_dev = [at(x, y, pz, core) for pz in z_at]

    barrier = pltpu.get_barrier_semaphore()
    peers = [up, down, halo, back, partner] + z_dev[1:]
    for peer in peers:
        pl.semaphore_signal(barrier, inc=1, device_id=peer, device_id_type=MESH)

    lane = lax.broadcasted_iota(jnp.int32, (1, 128), 1)
    raw[...] = jnp.full(raw.shape, -1, jnp.int32)
    raw[:tiles, :NB] = nb_ref[...]
    for t in range(tiles):
        n = count_ref[t]
        row = jnp.where(lane < jnp.minimum(n, NB), raw[t:t + 1, :], -1)
        raw[t:t + 1, :] = jnp.where(lane == NB, n, row)

    def rows_of(t):
        return x_ref[pl.ds(pl.multiple_of(t * TILE, TILE), TILE), :]

    def keys_values(t, carry):
        rows = rows_of(t)
        k = jnp.dot(rows, wk_ref[...], preferred_element_type=jnp.float32)
        for h in range(HEADS):
            kv_ref[h, t, 0] = jnp.transpose(k[:, h * HD:(h + 1) * HD]).astype(jnp.bfloat16)
        v = jnp.dot(rows, wv_ref[...], preferred_element_type=jnp.float32).astype(jnp.bfloat16)
        for h in range(HEADS):
            kv_ref[h, t, 1] = v[:, h * HD:(h + 1) * HD]
        return carry

    lax.fori_loop(0, tiles, keys_values, 0)
    kv_out[0, core, z] = kv_ref[z]
    pl.semaphore_wait(barrier, len(peers))

    live, shared = [], []

    def send(source, target, device):
        k = len(live)
        copy = pltpu.make_async_remote_copy(
            src_ref=source,
            dst_ref=target,
            send_sem=send_sem.at[k],
            recv_sem=recv_sem.at[k],
            device_id=device,
            device_id_type=MESH,
        )
        copy.start()
        live.append(copy)
        return copy

    def part(h):
        return pl.ds(h * half, half)

    def place(slot, u):
        return kv_out.at[slot, core, z_at[u[0]], part(u[1])]

    def share(slot, u, source=None):
        shared.append(send(place(slot, u) if source is None else source, place(slot, u), partner))

    own, relayed, q_in, raw_in = {}, {}, {}, {}
    above, below, far, halo_above, halo_below, passing = {}, {}, {}, {}, {}, {}

    def send_z(h):
        own[2, h] = send(kv_ref.at[z_at[1], part(h)], kv_out.at[0, core, z, part(h)], z_dev[1])
        own[1, h] = send(kv_ref.at[z_at[2], part(h)], kv_out.at[0, core, z, part(h)], z_dev[2])

    def spread(u, source):
        below[u] = send(source, place(2, u), up)
        above[u] = send(source, place(1, u), down)

    def straight(u):
        passing[u] = send(place(0, u), transit.at[DIRECT.index(u)], back)

    def cross(u):
        passing[u].wait_recv()
        spot = transit.at[DIRECT.index(u)]
        halo_below[u] = send(spot, place(5, u), up)
        halo_above[u] = send(spot, place(4, u), down)

    def arrived(u, fresh=True):
        above[u].wait_recv()
        if u[1] == 1:
            far[u] = send(place(1, u), place(3, u), down)
        if fresh:
            halo_above[u] = send(place(1, u), place(4, u), halo)
        share(1, u)
        below[u].wait_recv()
        if u[1] == 0:
            far[u] = send(place(2, u), place(3, u), up)
        if fresh:
            halo_below[u] = send(place(2, u), place(5, u), halo)
        share(2, u)

    def returned(u):
        halo_above[u].wait_recv()
        above[u] = send(place(4, u), place(1, u), back)
        share(4, u)
        halo_below[u].wait_recv()
        below[u] = send(place(5, u), place(2, u), back)
        share(5, u)

    def settle(u):
        halo_above[u].wait_recv()
        share(4, u)
        halo_below[u].wait_recv()
        share(5, u)

    def settle_far(u):
        far[u].wait_recv()
        share(3, u)

    def mine(u):
        own[u].wait_recv()
        share(0, u)

    send_z(0)
    spread((0, 0), kv_ref.at[z, part(0)])
    relayed[0] = send(kv_ref.at[z_at[3], part(0)], relay.at[0], z_dev[1])
    relayed[1] = send(kv_ref.at[z_at[3], part(1)], relay.at[1], z_dev[2])
    spread((0, 1), kv_ref.at[z, part(1)])
    send_z(1)
    share(0, (0, 0), kv_ref.at[z, part(0)])
    share(0, (0, 1), kv_ref.at[z, part(1)])

    def queries(t, carry):
        q = jnp.dot(rows_of(t), wq_ref[...], preferred_element_type=jnp.float32)
        q = q.astype(jnp.bfloat16)
        for h in range(HEADS):
            q_ref[h, t] = q[:, h * HD:(h + 1) * HD]
        return carry

    lax.fori_loop(0, tiles, queries, 0)
    q_out[z] = q_ref[z]
    raw_all[z] = raw[...]

    mine((1, 0))
    straight((1, 0))
    mine((2, 0))
    spread((2, 0), place(0, (2, 0)))
    relayed[0].wait_recv()
    own[3, 0] = send(relay.at[0], kv_out.at[0, core, z_at[2], part(0)], z_dev[1])
    relayed[1].wait_recv()
    own[3, 1] = send(relay.at[1], kv_out.at[0, core, z_at[1], part(1)], z_dev[2])
    for j, lands in ((1, 2), (2, 1), (3, 3)):
        raw_in[lands] = send(raw, raw_all.at[z], z_dev[j])
        q_in[lands] = send(q_ref.at[z_at[j]], q_out.at[z], z_dev[j])
    arrived((0, 0))
    arrived((0, 1))
    cross((1, 0))
    mine((1, 1))
    straight((1, 1))
    mine((2, 1))
    straight((2, 1))
    arrived((2, 0))
    mine((3, 0))
    spread((3, 0), place(0, (3, 0)))
    mine((3, 1))
    spread((3, 1), place(0, (3, 1)))
    returned((1, 0))
    settle_far((0, 0))
    settle((0, 0))
    cross((1, 1))
    cross((2, 1))
    arrived((3, 0))
    arrived((3, 1))
    arrived((1, 0), fresh=False)
    settle_far((0, 1))
    settle((0, 1))
    returned((1, 1))
    returned((2, 1))

    for j in (1, 2, 3):
        raw_in[j].wait_recv()
    lists = raw_all[...].reshape(ZD * raw.shape[0], 128)

    def look_up(i, found):
        return jnp.where(lists == i, valid_ref[i], found)

    found = lax.fori_loop(0, valid_ref.shape[0], look_up, jnp.zeros_like(lists))
    spot = jnp.maximum(lists, 0)
    relative = (spot // 64 + 9 - zone) % 8
    there_y = (spot // 32) % 2 * 2 + 1 - y_lo
    near = jnp.where((there_y + 4 - y) % 4 == 1, 1, 2)
    near = near + jnp.where(relative == 2 - 2 * y_lo, 0, 3)
    slot = jnp.where(relative == 1, jnp.where((spot // 32) % 2 == y_hi, 0, 3), near)
    code = ((slot * 2 + (spot // 4) % 2) * ZD + (spot // 8) % ZD) * 4 + spot % 4
    code = jnp.where(lists < 0, 0, code * 256 + found)
    code = jnp.where(lane == NB, lists, code)
    code_out[...] = jnp.zeros(code_out.shape, jnp.int32)
    for p in range(ZD):
        code_out[p * tiles:(p + 1) * tiles, :] = code[p * raw.shape[0]:p * raw.shape[0] + tiles]

    settle_far((2, 0))
    settle((2, 0))
    arrived((1, 1), fresh=False)
    arrived((2, 1), fresh=False)
    settle_far((1, 0))
    settle((3, 0))
    settle_far((3, 0))
    settle((3, 1))
    settle_far((3, 1))
    settle_far((1, 1))
    settle_far((2, 1))
    for c in shared + list(q_in.values()):
        c.wait_recv()
    for c in live:
        c.wait_send()


def exchange(lists, counts, valid, x, wq, wk, wv):
    tiles = x.shape[0] // TILE
    piece = (tiles, 2, TILE, HD)
    vmem, smem = pl.BlockSpec(memory_space=pltpu.VMEM), pl.BlockSpec(memory_space=pltpu.SMEM)
    return pl.pallas_call(
        exchange_kernel,
        out_shape=(
            jax.ShapeDtypeStruct((ZD * tiles + 8, 128), jnp.int32),
            jax.ShapeDtypeStruct((ZD, tiles, TILE, HD), x.dtype),
            jax.ShapeDtypeStruct((6, 2, ZD) + piece, x.dtype),
        ),
        in_specs=[vmem, smem, smem, vmem, vmem, vmem, vmem],
        out_specs=[vmem] * 3,
        scratch_shapes=[
            pltpu.VMEM((HEADS,) + piece, x.dtype),
            pltpu.VMEM((HEADS, tiles, TILE, HD), x.dtype),
            pltpu.VMEM((8, 128), jnp.int32),
            pltpu.VMEM((ZD, 8, 128), jnp.int32),
            pltpu.VMEM((2, tiles // 2) + piece[1:], x.dtype),
            pltpu.VMEM((len(DIRECT), tiles // 2) + piece[1:], x.dtype),
            pltpu.SemaphoreType.DMA((COPIES,)),
            pltpu.SemaphoreType.DMA((COPIES,)),
        ],
        compiler_params=pltpu.CompilerParams(
            collective_id=0, has_side_effects=True, vmem_limit_bytes=24 * 1024 * 1024
        ),
    )(lists, counts, valid, x, wq, wk, wv)


LEAD = 5


def attn_kernel(code_ref, q_ref, kv_ref, o_ref, s_even, s_odd, top_ref, den_ref, acc_ref):
    tiles = q_ref.shape[0]
    lane = lax.broadcasted_iota(jnp.int32, (1, TILE), 1)
    rings = (s_even, s_odd)

    def groups(i):
        return (code_ref[i, NB] + 7) // 8

    def advance(i, c):
        last = c + 1 >= groups(i)
        return jnp.where(last, jnp.minimum(i + 1, tiles), i), jnp.where(last, 0, c + 1)

    def scores(i, c, ring, slot):
        q = q_ref[jnp.minimum(i, tiles - 1)]
        top = jnp.where(c == 0, NEG, top_ref[i])
        for p in range(4):
            a = code_ref[i, c * 8 + 2 * p]
            b = code_ref[i, c * 8 + 2 * p + 1]
            keys = jnp.concatenate([kv_ref[a // 256, 0], kv_ref[b // 256, 0]], axis=1)
            s = jnp.dot(q, keys, preferred_element_type=jnp.float32)
            bias = jnp.concatenate(
                [jnp.where(lane < a % 256, 0.0, NEG), jnp.where(lane < b % 256, 0.0, NEG)],
                axis=1,
            )
            s = s + bias
            ring[slot, :, p * 256:(p + 1) * 256] = s
            top = jnp.maximum(top, jnp.maximum(s[:, :TILE], s[:, TILE:]))
        top_ref[i] = top

    def values(i, c, peak, ring, slot):
        den = jnp.where(c == 0, 0.0, den_ref[...])
        acc = jnp.where(c == 0, 0.0, acc_ref[...])
        ps, vs = [], []
        for p in range(4):
            a = code_ref[i, c * 8 + 2 * p]
            b = code_ref[i, c * 8 + 2 * p + 1]
            w = jnp.exp2((ring[slot, :, p * 256:(p + 1) * 256] - peak) * EXP_SCALE)
            den = den + (w[:, :TILE] + w[:, TILE:])
            ps.append(w.astype(jnp.bfloat16))
            vs += [kv_ref[a // 256, 1], kv_ref[b // 256, 1]]
        acc = acc + jnp.dot(
            jnp.concatenate(ps, axis=1),
            jnp.concatenate(vs, axis=0),
            preferred_element_type=jnp.float32,
        )
        den_ref[...] = den
        acc_ref[...] = acc
        o_ref[i] = (acc / jnp.sum(den, axis=1, keepdims=True)).astype(jnp.bfloat16)

    total = lax.fori_loop(0, tiles, lambda i, n: n + groups(i), 0)
    head = (jnp.int32(0), jnp.int32(0))
    for w in range(LEAD):
        scores(*head, rings[w % 2], w // 2)
        head = advance(*head)

    def pair(k, state):
        head, tail = state
        tails = (tail, advance(*tail))
        peaks = [jnp.max(top_ref[i], axis=1, keepdims=True) for i, _ in tails]
        for r in range(2):
            w = 2 * k + r
            scores(*head, rings[(r + LEAD) % 2], ((w + LEAD) // 2) % 4)
            values(*tails[r], peaks[r], rings[r], (w // 2) % 4)
            head = advance(*head)
        return head, advance(*tails[1])

    lax.fori_loop(0, (total + 1) // 2, pair, (head, (jnp.int32(0), jnp.int32(0))))


def attend(code, q, kv):
    tiles = q.shape[0]
    ring = pltpu.VMEM((4, TILE, 8 * TILE), jnp.float32)
    square = pltpu.VMEM((TILE, TILE), jnp.float32)
    return pl.pallas_call(
        attn_kernel,
        out_shape=jax.ShapeDtypeStruct((tiles + 1,) + q.shape[1:], jnp.bfloat16),
        in_specs=[
            pl.BlockSpec(memory_space=pltpu.SMEM),
            pl.BlockSpec(memory_space=pltpu.VMEM),
            pl.BlockSpec(memory_space=pltpu.VMEM),
        ],
        out_specs=pl.BlockSpec(memory_space=pltpu.VMEM),
        scratch_shapes=[
            ring, ring, pltpu.VMEM((tiles + 1, TILE, TILE), jnp.float32), square, square
        ],
        compiler_params=pltpu.CompilerParams(vmem_limit_bytes=24 * 1024 * 1024),
    )(code, q, kv)


def finish_kernel(
    o_ref, x_ref, wo_ref, wg_ref, wu_ref, wd_ref, out_ref,
    got, relay, res_ref, norm_ref, hid_ref, send_sem, recv_sem,
):
    zone, dev = lax.axis_index("zone"), lax.axis_index("dev")
    z = (dev // 2) % ZD
    tiles = x_ref.shape[0] // TILE
    half = tiles // 2
    z_at = [(z + d) % ZD for d in (1, 3, 2)]
    peers = [(zone, dev + 2 * (pz - z)) for pz in z_at[:2]]

    barrier = pltpu.get_barrier_semaphore()
    for peer in peers:
        pl.semaphore_signal(barrier, inc=1, device_id=peer, device_id_type=MESH)
    pl.semaphore_wait(barrier, len(peers))

    def send(k, source, target, device):
        copy = pltpu.make_async_remote_copy(
            src_ref=source,
            dst_ref=target,
            send_sem=send_sem.at[k],
            recv_sem=recv_sem.at[k],
            device_id=device,
            device_id_type=MESH,
        )
        copy.start()
        return copy

    hops = [
        send(h, o_ref.at[pl.ds(z_at[2] * tiles + h * half, half)], relay.at[h], peers[h])
        for h in range(2)
    ]
    ends = [
        send(2 + h, o_ref.at[pl.ds(z_at[h] * tiles, tiles)], got.at[1 - h], peers[h])
        for h in range(2)
    ]

    def add_head(head, piece):
        o = piece.reshape(tiles * TILE, HD)
        w = wo_ref[pl.ds(pl.multiple_of(head * HD, HD), HD), :]
        return jnp.dot(o, w, preferred_element_type=jnp.float32)

    res_ref[...] = x_ref[...].astype(jnp.float32) + add_head(
        z, o_ref[pl.ds(z * tiles, tiles)]
    )
    last = []
    for h in range(2):
        hops[h].wait_recv()
        last.append(send(4 + h, relay.at[h], got.at[2, pl.ds(h * half, half)], peers[h]))
    for h in range(2):
        ends[1 - h].wait_recv()
        res_ref[...] += add_head(z_at[h], got[h])
    for c in last:
        c.wait_recv()
    res_ref[...] += add_head(z_at[2], got[2])
    r = res_ref[...]
    inverse = lax.rsqrt(jnp.mean(r * r, axis=-1, keepdims=True) + 1e-06)
    norm_ref[...] = (r * inverse).astype(jnp.bfloat16)
    width = 256

    def hidden(f, carry):
        cols = pl.ds(pl.multiple_of(f * width, width), width)
        gate = jnp.dot(norm_ref[...], wg_ref[:, cols], preferred_element_type=jnp.float32)
        up = jnp.dot(norm_ref[...], wu_ref[:, cols], preferred_element_type=jnp.float32)
        hid_ref[:, cols] = (gate / (1.0 + jnp.exp(-gate)) * up).astype(jnp.bfloat16)
        return carry

    lax.fori_loop(0, wg_ref.shape[1] // width, hidden, 0)

    def down(f, carry):
        cols = pl.ds(pl.multiple_of(f * width, width), width)
        out_ref[:, cols] = (
            res_ref[:, cols]
            + jnp.dot(hid_ref[...], wd_ref[:, cols], preferred_element_type=jnp.float32)
        ).astype(jnp.bfloat16)
        return carry

    lax.fori_loop(0, D // width, down, 0)
    for c in hops + ends + last:
        c.wait_send()


def finish_layer(o, x, w_out, w_gate, w_up, w_down):
    rows = x.shape[0]
    tiles = rows // TILE
    ff = w_gate.shape[1]
    return pl.pallas_call(
        finish_kernel,
        out_shape=jax.ShapeDtypeStruct(x.shape, x.dtype),
        in_specs=[pl.BlockSpec(memory_space=pltpu.VMEM)] * 6,
        out_specs=pl.BlockSpec(memory_space=pltpu.VMEM),
        scratch_shapes=[
            pltpu.VMEM((ZD - 1, tiles, TILE, HD), jnp.bfloat16),
            pltpu.VMEM((2, tiles // 2, TILE, HD), jnp.bfloat16),
            pltpu.VMEM(x.shape, jnp.float32),
            pltpu.VMEM(x.shape, jnp.bfloat16),
            pltpu.VMEM((rows, ff), jnp.bfloat16),
            pltpu.SemaphoreType.DMA((6,)),
            pltpu.SemaphoreType.DMA((6,)),
        ],
        compiler_params=pltpu.CompilerParams(
            collective_id=1, has_side_effects=True, vmem_limit_bytes=24 * 1024 * 1024
        ),
    )(o, x, w_out, w_gate, w_up, w_down)


def body(
    x,
    neighbour_blocks,
    neighbour_count,
    tile_valid,
    w_query,
    w_key,
    w_value,
    w_out,
    w_gate,
    w_up,
    w_down,
):
    tiles = x.shape[0] // TILE
    codes, q, kv = exchange(
        neighbour_blocks, neighbour_count, tile_valid, x, w_query, w_key, w_value
    )
    o = attend(
        codes, q.reshape(ZD * tiles, TILE, HD), kv.reshape(6 * 2 * ZD * tiles, 2, TILE, HD)
    )
    return finish_layer(o, x, w_out, w_gate, w_up, w_down)


def solution(mesh):
    placed = (
        P(("zone", "dev"), None),
        P(("zone", "dev"), None),
        P(("zone", "dev")),
        P(),
        P(),
        P(),
        P(),
        P(),
        P(),
        P(),
        P(),
    )
    return jax.shard_map(
        body, mesh=mesh, in_specs=placed, out_specs=P(("zone", "dev"), None), check_vma=False
    )
```

```python
import math

import jax
import jax.numpy as jnp
from jax import lax
from jax.experimental import pallas as pl
from jax.experimental.pallas import tpu as pltpu
from jax.sharding import PartitionSpec as P

D = 512
HEADS = 4
HD = 128
TILE = 128
NB = 32
ZD = 4
NEG = -1e30
EXP_SCALE = math.log2(math.e) / math.sqrt(HD)


MESH = pl.DeviceIdType.MESH
UNITS = tuple((j, h) for j in range(ZD) for h in range(2))
DIRECT = ((1, 0), (1, 1), (2, 1))
COPIES = 112
ORDER = (3, 1, 2, 0)


def layer_kernel(
    nb_hbm, count_hbm, valid_hbm, x_hbm, wq_hbm, wk_hbm, wv_hbm, wo_hbm, wg_hbm, wu_hbm, wd_hbm,
    out_ref,
    nb_ref, count_ref, valid_ref, x_ref, wq_ref, wk_ref, wv_ref, wo_ref, wg_ref, wu_ref, wd_ref,
    kv_out, q_out, kv_ref, q_ref, raw, raw_all, relay, transit, code_vec, code_ref,
    s_even, s_odd, p_even, p_odd, d_even, d_odd, t_even, t_odd,
    o_ref, got, hop, res_ref, norm_ref, hid_ref,
    load_sem, send_sem, recv_sem,
):
    zone, dev = lax.axis_index("zone"), lax.axis_index("dev")
    x, y_lo = zone // 2, zone % 2
    y_hi, z, core = dev // 8, (dev // 2) % ZD, dev % 2
    y = y_hi * 2 + y_lo
    tiles = x_ref.shape[0] // TILE
    half = tiles // 2

    def at(px, py, pz, pc):
        return (px * 2 + py % 2, (py // 2) * 8 + pz * 2 + pc)

    side = 1 - 2 * y_lo
    up, down = at(x, (y + 1) % 4, z, core), at(x, (y + 3) % 4, z, core)
    halo, back = at((x + 4 + side) % 4, y, z, core), at((x + 4 - side) % 4, y, z, core)
    partner = at(x, y, z, 1 - core)
    z_at = [(z + d) % ZD for d in (0, 1, 3, 2)]
    z_dev = [at(x, y, pz, core) for pz in z_at]

    barrier = pltpu.get_barrier_semaphore()
    peers = [up, down, halo, back, partner] + z_dev[1:]
    for peer in peers:
        pl.semaphore_signal(barrier, inc=1, device_id=peer, device_id_type=MESH)

    loads = [
        pltpu.make_async_copy(source, target, load_sem.at[i])
        for i, (source, target) in enumerate(
            (
                (x_hbm, x_ref), (wk_hbm, wk_ref), (wv_hbm, wv_ref), (nb_hbm, nb_ref),
                (count_hbm, count_ref), (wq_hbm, wq_ref), (valid_hbm, valid_ref),
                (wo_hbm, wo_ref), (wg_hbm, wg_ref), (wu_hbm, wu_ref), (wd_hbm, wd_ref),
            )
        )
    ]
    for c in loads:
        c.start()
    for c in loads[:5]:
        c.wait()

    lane = lax.broadcasted_iota(jnp.int32, (1, 128), 1)
    raw[...] = jnp.full(raw.shape, -1, jnp.int32)
    raw[:tiles, :NB] = nb_ref[...]
    for t in range(tiles):
        n = count_ref[t]
        row = jnp.where(lane < jnp.minimum(n, NB), raw[t:t + 1, :], -1)
        raw[t:t + 1, :] = jnp.where(lane == NB, n, row)

    def rows_of(t):
        return x_ref[pl.ds(pl.multiple_of(t * TILE, TILE), TILE), :]

    def keys_values(t, carry):
        rows = rows_of(t)
        k = jnp.dot(rows, wk_ref[...], preferred_element_type=jnp.float32)
        for h in range(HEADS):
            kv_ref[h, t, 0] = jnp.transpose(k[:, h * HD:(h + 1) * HD]).astype(jnp.bfloat16)
        v = jnp.dot(rows, wv_ref[...], preferred_element_type=jnp.float32).astype(jnp.bfloat16)
        for h in range(HEADS):
            kv_ref[h, t, 1] = v[:, h * HD:(h + 1) * HD]
        return carry

    lax.fori_loop(0, tiles, keys_values, 0)
    kv_out[pl.ds((core * ZD + z) * tiles, tiles)] = kv_ref[z]
    pl.semaphore_wait(barrier, len(peers))

    live, shared = [], []

    def send(source, target, device):
        k = len(live)
        copy = pltpu.make_async_remote_copy(
            src_ref=source,
            dst_ref=target,
            send_sem=send_sem.at[k],
            recv_sem=recv_sem.at[k],
            device_id=device,
            device_id_type=MESH,
        )
        copy.start()
        live.append(copy)
        return copy

    def part(h):
        return pl.ds(h * half, half)

    def spot_of(slot, pz, h):
        return kv_out.at[pl.ds(((slot * 2 + core) * ZD + pz) * tiles + h * half, half)]

    def place(slot, u):
        return spot_of(slot, z_at[u[0]], u[1])

    def share(slot, u, source=None):
        shared.append(send(place(slot, u) if source is None else source, place(slot, u), partner))

    own, relayed, q_in, raw_in = {}, {}, {}, {}
    above, below, far, halo_above, halo_below, passing = {}, {}, {}, {}, {}, {}

    def send_z(h):
        own[2, h] = send(kv_ref.at[z_at[1], part(h)], spot_of(0, z, h), z_dev[1])
        own[1, h] = send(kv_ref.at[z_at[2], part(h)], spot_of(0, z, h), z_dev[2])

    def spread(u, source):
        below[u] = send(source, place(2, u), up)
        above[u] = send(source, place(1, u), down)

    def straight(u):
        passing[u] = send(place(0, u), transit.at[DIRECT.index(u)], back)

    def cross(u):
        passing[u].wait_recv()
        spot = transit.at[DIRECT.index(u)]
        halo_below[u] = send(spot, place(5, u), up)
        halo_above[u] = send(spot, place(4, u), down)

    def arrived(u, fresh=True):
        above[u].wait_recv()
        if u[1] == 1:
            far[u] = send(place(1, u), place(3, u), down)
        if fresh:
            halo_above[u] = send(place(1, u), place(4, u), halo)
        share(1, u)
        below[u].wait_recv()
        if u[1] == 0:
            far[u] = send(place(2, u), place(3, u), up)
        if fresh:
            halo_below[u] = send(place(2, u), place(5, u), halo)
        share(2, u)

    def returned(u):
        halo_above[u].wait_recv()
        above[u] = send(place(4, u), place(1, u), back)
        share(4, u)
        halo_below[u].wait_recv()
        below[u] = send(place(5, u), place(2, u), back)
        share(5, u)

    def settle(u):
        halo_above[u].wait_recv()
        share(4, u)
        halo_below[u].wait_recv()
        share(5, u)

    def settle_far(u):
        far[u].wait_recv()
        share(3, u)

    def mine(u):
        own[u].wait_recv()
        share(0, u)

    send_z(0)
    spread((0, 0), kv_ref.at[z, part(0)])
    relayed[0] = send(kv_ref.at[z_at[3], part(0)], relay.at[0], z_dev[1])
    relayed[1] = send(kv_ref.at[z_at[3], part(1)], relay.at[1], z_dev[2])
    spread((0, 1), kv_ref.at[z, part(1)])
    send_z(1)
    share(0, (0, 0), kv_ref.at[z, part(0)])
    share(0, (0, 1), kv_ref.at[z, part(1)])

    def queries(t, carry):
        q = jnp.dot(rows_of(t), wq_ref[...], preferred_element_type=jnp.float32)
        q = q.astype(jnp.bfloat16)
        for h in range(HEADS):
            q_ref[h, t] = q[:, h * HD:(h + 1) * HD]
        return carry

    loads[5].wait()
    lax.fori_loop(0, tiles, queries, 0)
    q_out[z] = q_ref[z]
    raw_all[z] = raw[...]

    mine((1, 0))
    straight((1, 0))
    mine((2, 0))
    spread((2, 0), place(0, (2, 0)))
    relayed[0].wait_recv()
    own[3, 0] = send(relay.at[0], spot_of(0, z_at[2], 0), z_dev[1])
    relayed[1].wait_recv()
    own[3, 1] = send(relay.at[1], spot_of(0, z_at[1], 1), z_dev[2])
    for j, lands in ((1, 2), (2, 1), (3, 3)):
        raw_in[lands] = send(raw, raw_all.at[z], z_dev[j])
        q_in[lands] = send(q_ref.at[z_at[j]], q_out.at[z], z_dev[j])
    arrived((0, 0))
    arrived((0, 1))
    cross((1, 0))
    mine((1, 1))
    straight((1, 1))
    mine((2, 1))
    straight((2, 1))
    arrived((2, 0))
    mine((3, 0))
    spread((3, 0), place(0, (3, 0)))
    mine((3, 1))
    spread((3, 1), place(0, (3, 1)))
    returned((1, 0))
    settle_far((0, 0))
    settle((0, 0))
    cross((1, 1))
    cross((2, 1))
    arrived((3, 0))
    arrived((3, 1))
    arrived((1, 0), fresh=False)
    settle_far((0, 1))
    settle((0, 1))
    returned((1, 1))
    returned((2, 1))

    for j in (1, 2, 3):
        raw_in[j].wait_recv()
    lists = raw_all[...].reshape(ZD * raw.shape[0], 128)

    loads[6].wait()

    def look_up(i, found):
        return jnp.where(lists == i, valid_ref[i], found)

    found = lax.fori_loop(0, valid_ref.shape[0], look_up, jnp.zeros_like(lists))
    spot = jnp.maximum(lists, 0)
    relative = (spot // 64 + 9 - zone) % 8
    there_y = (spot // 32) % 2 * 2 + 1 - y_lo
    near = jnp.where((there_y + 4 - y) % 4 == 1, 1, 2)
    near = near + jnp.where(relative == 2 - 2 * y_lo, 0, 3)
    slot = jnp.where(relative == 1, jnp.where((spot // 32) % 2 == y_hi, 0, 3), near)
    code = ((slot * 2 + (spot // 4) % 2) * ZD + (spot // 8) % ZD) * 4 + spot % 4
    code = jnp.where(lists < 0, 0, code * 256 + found)
    code = jnp.where(lane == NB, lists, code)
    for p in range(ZD):
        code_vec[p * tiles:(p + 1) * tiles, :] = code[p * raw.shape[0]:p * raw.shape[0] + tiles]

    to_smem = pltpu.make_async_copy(code_vec, code_ref, load_sem.at[11])
    to_smem.start()
    settle_far((2, 0))
    settle((2, 0))
    arrived((1, 1), fresh=False)
    arrived((2, 1), fresh=False)
    settle_far((1, 0))
    settle((3, 0))
    settle_far((3, 0))
    settle((3, 1))
    settle_far((3, 1))
    settle_far((1, 1))
    settle_far((2, 1))
    for c in shared + list(q_in.values()):
        c.wait_recv()
    to_smem.wait()

    s_bufs, p_bufs = (s_even, s_odd), (p_even, p_odd)
    d_bufs, t_bufs = (d_even, d_odd), (t_even, t_odd)
    count = ZD * tiles

    def owner(n):
        g = n // tiles
        d = jnp.where(g == 0, 2, jnp.where(g == 1, 1, jnp.where(g == 2, 3, 0)))
        return (z + d) % ZD

    def scores(n, b):
        pz, t = owner(n), n % tiles
        i = pz * tiles + t
        q = q_out[pz, t]
        top = None
        for p in range(NB // 2):
            e, f = code_ref[i, 2 * p], code_ref[i, 2 * p + 1]
            keys = jnp.concatenate([kv_out[e // 256, 0], kv_out[f // 256, 0]], axis=1)
            s = jnp.dot(q, keys, preferred_element_type=jnp.float32)
            bias = jnp.concatenate(
                [jnp.where(lane < e % 256, 0.0, NEG), jnp.where(lane < f % 256, 0.0, NEG)],
                axis=1,
            )
            s = s + bias
            s_bufs[b][:, p * 256:(p + 1) * 256] = s
            pair_top = jnp.maximum(s[:, :TILE], s[:, TILE:])
            top = pair_top if top is None else jnp.maximum(top, pair_top)
        t_bufs[b][...] = top

    def weights(b):
        for g in range(TILE // 16):
            rows = slice(g * 16, (g + 1) * 16)
            peak = jnp.max(t_bufs[b][rows, :], axis=1, keepdims=True)
            den = None
            for k in range(NB):
                cols = slice(k * TILE, (k + 1) * TILE)
                w = jnp.exp2((s_bufs[b][rows, cols] - peak) * EXP_SCALE)
                den = w if den is None else den + w
                p_bufs[b][rows, cols] = w.astype(jnp.bfloat16)
            total = jnp.sum(den, axis=1, keepdims=True)
            d_bufs[b][rows, :] = jnp.broadcast_to(1.0 / total, (16, TILE))

    def values(n, b):
        i = owner(n) * tiles + n % tiles
        v = jnp.concatenate([kv_out[code_ref[i, p] // 256, 1] for p in range(NB)], axis=0)
        acc = jnp.dot(p_bufs[b][...], v, preferred_element_type=jnp.float32)
        o_ref[n] = (acc * d_bufs[b][...]).astype(jnp.bfloat16)

    base = len(live)

    def describe(k, source, target, device):
        return pltpu.make_async_remote_copy(
            src_ref=source,
            dst_ref=target,
            send_sem=send_sem.at[base + k],
            recv_sem=recv_sem.at[base + k],
            device_id=device,
            device_id_type=MESH,
        )

    hops = [
        describe(h, o_ref.at[pl.ds(h * half, half)], hop.at[h], z_dev[1 + h]) for h in range(2)
    ]
    ends = [
        describe(2 + h, o_ref.at[pl.ds((1 + h) * tiles, tiles)], got.at[1 - h], z_dev[1 + h])
        for h in range(2)
    ]
    last = [
        describe(4 + h, hop.at[h], got.at[2, part(h)], z_dev[1 + h]) for h in range(2)
    ]

    scores(jnp.int32(0), 0)
    scores(jnp.int32(1), 1)
    weights(0)

    def pair(k, carry):
        for r in range(2):
            n = 2 * k + r
            values(n, r)
            scores(n + 2, r)
            weights(1 - r)

        @pl.when(k == 2)
        def _():
            for c in hops:
                c.start()

        @pl.when(k == 4)
        def _():
            ends[0].start()

        @pl.when(k == 5)
        def _():
            for c, d in zip(hops, last):
                c.wait_recv()
                d.start()

        @pl.when(k == 6)
        def _():
            ends[1].start()

        return carry

    lax.fori_loop(0, count // 2 - 1, pair, 0)
    values(jnp.int32(count - 2), 0)
    weights(1)
    values(jnp.int32(count - 1), 1)

    def add_head(pz, piece):
        o = piece.reshape(tiles * TILE, HD)
        w = wo_ref[pl.ds(pl.multiple_of(pz * HD, HD), HD), :]
        return jnp.dot(o, w, preferred_element_type=jnp.float32)

    for c in loads[7:]:
        c.wait()
    res_ref[...] = x_ref[...].astype(jnp.float32) + add_head(z, o_ref[3 * tiles:])
    for c in last:
        c.wait_recv()
    res_ref[...] += add_head(z_at[3], got[2])
    for h in (1, 0):
        ends[1 - h].wait_recv()
        res_ref[...] += add_head(z_at[1 + h], got[h])
    r = res_ref[...]
    inverse = lax.rsqrt(jnp.mean(r * r, axis=-1, keepdims=True) + 1e-06)
    norm_ref[...] = (r * inverse).astype(jnp.bfloat16)
    width = 256

    def hidden(f, carry):
        cols = pl.ds(pl.multiple_of(f * width, width), width)
        gate = jnp.dot(norm_ref[...], wg_ref[:, cols], preferred_element_type=jnp.float32)
        lift = jnp.dot(norm_ref[...], wu_ref[:, cols], preferred_element_type=jnp.float32)
        hid_ref[:, cols] = (gate / (1.0 + jnp.exp(-gate)) * lift).astype(jnp.bfloat16)
        return carry

    lax.fori_loop(0, wg_ref.shape[1] // width, hidden, 0)

    def lower(f, carry):
        cols = pl.ds(pl.multiple_of(f * width, width), width)
        out_ref[:, cols] = (
            res_ref[:, cols]
            + jnp.dot(hid_ref[...], wd_ref[:, cols], preferred_element_type=jnp.float32)
        ).astype(jnp.bfloat16)
        return carry

    lax.fori_loop(0, D // width, lower, 0)
    for c in live + hops + ends + last:
        c.wait_send()


def body(
    x, lists, counts, valid, w_query, w_key, w_value, w_out, w_gate, w_up, w_down
):
    tiles = x.shape[0] // TILE
    piece = (tiles, 2, TILE, HD)
    weights = (w_query, w_key, w_value, w_out, w_gate, w_up, w_down)
    copied = (x,) + weights

    def fast(shape, dtype=x.dtype):
        return pltpu.VMEM(shape, dtype)

    return pl.pallas_call(
        layer_kernel,
        out_shape=jax.ShapeDtypeStruct(x.shape, x.dtype),
        in_specs=[pl.BlockSpec(memory_space=pltpu.HBM)] * 11,
        out_specs=pl.BlockSpec(memory_space=pltpu.VMEM),
        scratch_shapes=[
            fast(lists.shape, jnp.int32),
            pltpu.SMEM(counts.shape, jnp.int32),
            pltpu.SMEM(valid.shape, jnp.int32),
        ]
        + [fast(a.shape) for a in copied]
        + [
            fast((6 * 2 * ZD * tiles,) + piece[1:]),
            fast((ZD, tiles, TILE, HD)),
            fast((HEADS,) + piece),
            fast((HEADS, tiles, TILE, HD)),
            fast((8, 128), jnp.int32),
            fast((ZD, 8, 128), jnp.int32),
            fast((2, tiles // 2) + piece[1:]),
            fast((len(DIRECT), tiles // 2) + piece[1:]),
            fast((ZD * tiles, 128), jnp.int32),
            pltpu.SMEM((ZD * tiles, 128), jnp.int32),
        ]
        + [fast((TILE, NB * TILE), jnp.float32)] * 2
        + [fast((TILE, NB * TILE))] * 2
        + [fast((TILE, TILE), jnp.float32)] * 4
        + [
            fast((ZD * tiles, TILE, HD)),
            fast((ZD - 1, tiles, TILE, HD)),
            fast((2, tiles // 2, TILE, HD)),
            fast(x.shape, jnp.float32),
            fast(x.shape),
            fast((x.shape[0], w_gate.shape[1])),
            pltpu.SemaphoreType.DMA((12,)),
            pltpu.SemaphoreType.DMA((COPIES,)),
            pltpu.SemaphoreType.DMA((COPIES,)),
        ],
        compiler_params=pltpu.CompilerParams(
            collective_id=0, has_side_effects=True, vmem_limit_bytes=67043328
        ),
    )(lists, counts, valid, x, *weights)


def solution(mesh):
    placed = (
        P(("zone", "dev"), None),
        P(("zone", "dev"), None),
        P(("zone", "dev")),
        P(),
        P(),
        P(),
        P(),
        P(),
        P(),
        P(),
        P(),
    )
    return jax.shard_map(
        body, mesh=mesh, in_specs=placed, out_specs=P(("zone", "dev"), None), check_vma=False
    )
```

```python
import heapq
import math

import jax
import jax.numpy as jnp
from jax import lax
from jax.experimental import pallas as pl
from jax.experimental.pallas import tpu as pltpu
from jax.sharding import PartitionSpec as P

D = 512
HEADS = 4
HD = 128
TILE = 128
NB = 32
ZD = 4
NEG = -1e30
EXP_SCALE = math.log2(math.e) / math.sqrt(HD)


MESH = pl.DeviceIdType.MESH
PARTS = 4
DIRECT = ((1, 0), (1, 1), (1, 2), (1, 3), (2, 0), (2, 2))
OPENING = (("own", 0), ("next", 1), ("next", 3), ("relay", 1), ("next", 2), ("relay", 2), ("own", 3), ("own", 2), ("next", 0), ("relay", 3), ("own", 1), ("relay", 0))
FAR_UP = ((0, 0), (1, 0), (1, 2), (2, 0), (2, 3), (3, 0), (3, 1), (3, 3))


COPIES = 210


def arrivals():
    unit, hop = 5.6 / PARTS, 3.1
    free, events, order = {}, [], []

    def send(now, key, link):
        free[link] = max(now, free.get(link, 0.0)) + unit
        heapq.heappush(events, (free[link] + hop, len(order) + len(events), key))

    def own(now, u):
        if u in DIRECT:
            send(now, ("transit", u), "back")
        else:
            send(now, ("below", u), "up")
            send(now, ("above", u), "down")

    for kind, h in OPENING:
        if kind == "own":
            own(0.0, (0, h))
        elif kind == "next":
            send(0.0, ("own", (2, h)), "next")
            send(0.0, ("own", (1, h)), "prior")
        else:
            send(0.0, ("relay", h), "next" if 2 * h < PARTS else "prior")
    while events:
        now, _, (kind, u) = heapq.heappop(events)
        order.append((kind, u))
        if kind == "own":
            own(now, u)
        elif kind == "relay":
            send(now, ("own", (3, u)), "next" if 2 * u < PARTS else "prior")
        elif kind == "transit":
            send(now, ("halo_below", u), "up")
            send(now, ("halo_above", u), "down")
        elif kind in ("above", "below"):
            if (kind == "below") == (u in FAR_UP):
                send(now, ("far", u), "up" if kind == "below" else "down")
            if u not in DIRECT:
                send(now, ("halo_" + kind, u), "halo")
        elif kind in ("halo_above", "halo_below") and u in DIRECT:
            send(now, (kind[5:], u), "back")
    return order


def layer_kernel(
    nb_hbm, count_hbm, valid_hbm, x_hbm, wq_hbm, wk_hbm, wv_hbm, wo_hbm, wg_hbm, wu_hbm, wd_hbm,
    out_ref,
    nb_ref, count_ref, valid_ref, x_ref, wq_ref, wk_ref, wv_ref, wo_ref, wg_ref, wu_ref, wd_ref,
    kv_out, q_out, kv_ref, q_ref, raw, raw_all, relay, transit, code_vec, code_ref,
    s_even, s_odd, p_even, p_odd, d_even, d_odd, t_even, t_odd,
    o_ref, got, hop, res_ref, norm_ref, hid_ref,
    load_sem, send_sem, recv_sem,
):
    zone, dev = lax.axis_index("zone"), lax.axis_index("dev")
    x, y_lo = zone // 2, zone % 2
    y_hi, z, core = dev // 8, (dev // 2) % ZD, dev % 2
    y = y_hi * 2 + y_lo
    tiles = x_ref.shape[0] // TILE
    size = tiles // PARTS
    half = tiles // 2

    def at(px, py, pz, pc):
        return (px * 2 + py % 2, (py // 2) * 8 + pz * 2 + pc)

    side = 1 - 2 * y_lo
    up, down = at(x, (y + 1) % 4, z, core), at(x, (y + 3) % 4, z, core)
    halo, back = at((x + 4 + side) % 4, y, z, core), at((x + 4 - side) % 4, y, z, core)
    partner = at(x, y, z, 1 - core)
    z_at = [(z + d) % ZD for d in (0, 1, 3, 2)]
    z_dev = [at(x, y, pz, core) for pz in z_at]

    barrier = pltpu.get_barrier_semaphore()
    peers = [up, down, halo, back, partner] + z_dev[1:]
    for peer in peers:
        pl.semaphore_signal(barrier, inc=1, device_id=peer, device_id_type=MESH)

    loads = [
        pltpu.make_async_copy(source, target, load_sem.at[i])
        for i, (source, target) in enumerate(
            (
                (x_hbm, x_ref), (wk_hbm, wk_ref), (wv_hbm, wv_ref), (nb_hbm, nb_ref),
                (count_hbm, count_ref), (wq_hbm, wq_ref), (valid_hbm, valid_ref),
                (wo_hbm, wo_ref), (wg_hbm, wg_ref), (wu_hbm, wu_ref), (wd_hbm, wd_ref),
            )
        )
    ]
    for c in loads:
        c.start()
    for c in loads[:5]:
        c.wait()

    lane = lax.broadcasted_iota(jnp.int32, (1, 128), 1)
    raw[...] = jnp.full(raw.shape, -1, jnp.int32)
    raw[:tiles, :NB] = nb_ref[...]
    for t in range(tiles):
        n = count_ref[t]
        row = jnp.where(lane < jnp.minimum(n, NB), raw[t:t + 1, :], -1)
        raw[t:t + 1, :] = jnp.where(lane == NB, n, row)

    def rows_of(t):
        return x_ref[pl.ds(pl.multiple_of(t * TILE, TILE), TILE), :]

    def keys_values(t, carry):
        rows = rows_of(t)
        k = jnp.dot(rows, wk_ref[...], preferred_element_type=jnp.float32)
        for h in range(HEADS):
            kv_ref[h, t, 0] = jnp.transpose(k[:, h * HD:(h + 1) * HD]).astype(jnp.bfloat16)
        v = jnp.dot(rows, wv_ref[...], preferred_element_type=jnp.float32).astype(jnp.bfloat16)
        for h in range(HEADS):
            kv_ref[h, t, 1] = v[:, h * HD:(h + 1) * HD]
        return carry

    lax.fori_loop(0, tiles, keys_values, 0)
    kv_out[pl.ds((core * ZD + z) * tiles, tiles)] = kv_ref[z]
    pl.semaphore_wait(barrier, len(peers))

    live, flying, shared = [], {}, []

    def send(source, target, device):
        k = len(live)
        copy = pltpu.make_async_remote_copy(
            src_ref=source,
            dst_ref=target,
            send_sem=send_sem.at[k],
            recv_sem=recv_sem.at[k],
            device_id=device,
            device_id_type=MESH,
        )
        copy.start()
        live.append(copy)
        return copy

    def part(h):
        return pl.ds(h * size, size)

    def spot_of(slot, pz, h):
        return kv_out.at[pl.ds(((slot * 2 + core) * ZD + pz) * tiles + h * size, size)]

    def place(slot, u):
        return spot_of(slot, z_at[u[0]], u[1])

    def share(slot, u, source=None):
        shared.append(send(place(slot, u) if source is None else source, place(slot, u), partner))

    def own(u, source):
        if u in DIRECT:
            flying["transit", u] = send(source, transit.at[DIRECT.index(u)], back)
        else:
            flying["below", u] = send(source, place(2, u), up)
            flying["above", u] = send(source, place(1, u), down)
        share(0, u, source)

    def forward(kind, u):
        flying[kind, u].wait_recv()
        if kind == "own":
            own(u, place(0, u))
        elif kind == "relay":
            along = 2 * u < PARTS
            flying["own", (3, u)] = send(
                relay.at[u], spot_of(0, z_at[2 if along else 1], u), z_dev[1 if along else 2]
            )
        elif kind == "transit":
            spot = transit.at[DIRECT.index(u)]
            flying["halo_below", u] = send(spot, place(5, u), up)
            flying["halo_above", u] = send(spot, place(4, u), down)
        elif kind in ("above", "below"):
            slot = 1 if kind == "above" else 2
            if (kind == "below") == (u in FAR_UP):
                flying["far", u] = send(
                    place(slot, u), place(3, u), up if kind == "below" else down
                )
            if u not in DIRECT:
                flying["halo_" + kind, u] = send(place(slot, u), place(slot + 3, u), halo)
            share(slot, u)
        elif kind == "far":
            share(3, u)
        else:
            slot = 4 if kind == "halo_above" else 5
            if u in DIRECT:
                flying[kind[5:], u] = send(place(slot, u), place(slot - 3, u), back)
            share(slot, u)

    for kind, h in OPENING:
        if kind == "own":
            own((0, h), kv_ref.at[z, part(h)])
        elif kind == "next":
            flying["own", (2, h)] = send(
                kv_ref.at[z_at[1], part(h)], spot_of(0, z, h), z_dev[1]
            )
            flying["own", (1, h)] = send(
                kv_ref.at[z_at[2], part(h)], spot_of(0, z, h), z_dev[2]
            )
        else:
            flying["relay", h] = send(
                kv_ref.at[z_at[3], part(h)], relay.at[h], z_dev[1 if 2 * h < PARTS else 2]
            )

    def queries(t, carry):
        q = jnp.dot(rows_of(t), wq_ref[...], preferred_element_type=jnp.float32)
        q = q.astype(jnp.bfloat16)
        for h in range(HEADS):
            q_ref[h, t] = q[:, h * HD:(h + 1) * HD]
        return carry

    loads[5].wait()
    lax.fori_loop(0, tiles, queries, 0)
    q_out[z] = q_ref[z]
    raw_all[z] = raw[...]

    order = arrivals()
    relays = [n for n, (kind, _) in enumerate(order) if kind == "relay"]
    middle = 2 * len(order) // 3
    for kind, u in order[:relays[-1] + 1]:
        forward(kind, u)
    q_in, raw_in = {}, {}
    for j, lands in ((1, 2), (2, 1), (3, 3)):
        raw_in[lands] = send(raw, raw_all.at[z], z_dev[j])
        q_in[lands] = send(q_ref.at[z_at[j]], q_out.at[z], z_dev[j])
    for kind, u in order[relays[-1] + 1:middle]:
        forward(kind, u)

    for j in (1, 2, 3):
        raw_in[j].wait_recv()
    lists = raw_all[...].reshape(ZD * raw.shape[0], 128)

    loads[6].wait()

    span = 3 * 64

    def look_up(i, found):
        g = (zone * 64 + valid_ref.shape[0] - 64 + i) % valid_ref.shape[0]
        return jnp.where(lists == g, valid_ref[g], found)

    found = lax.fori_loop(0, span, look_up, jnp.zeros_like(lists), unroll=8)
    spot = jnp.maximum(lists, 0)
    relative = (spot // 64 + 9 - zone) % 8
    there_y = (spot // 32) % 2 * 2 + 1 - y_lo
    near = jnp.where((there_y + 4 - y) % 4 == 1, 1, 2)
    near = near + jnp.where(relative == 2 - 2 * y_lo, 0, 3)
    slot = jnp.where(relative == 1, jnp.where((spot // 32) % 2 == y_hi, 0, 3), near)
    code = ((slot * 2 + (spot // 4) % 2) * ZD + (spot // 8) % ZD) * 4 + spot % 4
    code = jnp.where(lists < 0, 0, code * 256 + found)
    code = jnp.where(lane == NB, lists, code)
    for p in range(ZD):
        code_vec[p * tiles:(p + 1) * tiles, :] = code[p * raw.shape[0]:p * raw.shape[0] + tiles]

    to_smem = pltpu.make_async_copy(code_vec, code_ref, load_sem.at[11])
    to_smem.start()
    for kind, u in order[middle:]:
        forward(kind, u)
    for c in shared + list(q_in.values()):
        c.wait_recv()
    to_smem.wait()

    s_bufs, p_bufs = (s_even, s_odd), (p_even, p_odd)
    d_bufs, t_bufs = (d_even, d_odd), (t_even, t_odd)
    count = ZD * tiles

    def owner(n):
        g = n // tiles
        d = jnp.where(g == 0, 2, jnp.where(g == 1, 1, jnp.where(g == 2, 3, 0)))
        return (z + d) % ZD

    def scores(n, b):
        pz, t = owner(n), n % tiles
        i = pz * tiles + t
        q = q_out[pz, t]
        top = None
        for p in range(NB // 2):
            e, f = code_ref[i, 2 * p], code_ref[i, 2 * p + 1]
            keys = jnp.concatenate([kv_out[e // 256, 0], kv_out[f // 256, 0]], axis=1)
            s = jnp.dot(q, keys, preferred_element_type=jnp.float32)
            bias = jnp.concatenate(
                [jnp.where(lane < e % 256, 0.0, NEG), jnp.where(lane < f % 256, 0.0, NEG)],
                axis=1,
            )
            s = s + bias
            s_bufs[b][:, p * 256:(p + 1) * 256] = s
            pair_top = jnp.maximum(s[:, :TILE], s[:, TILE:])
            top = pair_top if top is None else jnp.maximum(top, pair_top)
        t_bufs[b][...] = top

    def weights(b):
        for g in range(TILE // 16):
            rows = slice(g * 16, (g + 1) * 16)
            peak = jnp.max(t_bufs[b][rows, :], axis=1, keepdims=True)
            den = None
            for k in range(NB):
                cols = slice(k * TILE, (k + 1) * TILE)
                w = jnp.exp2((s_bufs[b][rows, cols] - peak) * EXP_SCALE)
                den = w if den is None else den + w
                p_bufs[b][rows, cols] = w.astype(jnp.bfloat16)
            total = jnp.sum(den, axis=1, keepdims=True)
            d_bufs[b][rows, :] = jnp.broadcast_to(1.0 / total, (16, TILE))

    def values(n, b):
        i = owner(n) * tiles + n % tiles
        v = jnp.concatenate([kv_out[code_ref[i, p] // 256, 1] for p in range(NB)], axis=0)
        acc = jnp.dot(p_bufs[b][...], v, preferred_element_type=jnp.float32)
        o_ref[n] = (acc * d_bufs[b][...]).astype(jnp.bfloat16)

    base = len(live)

    def describe(k, source, target, device):
        return pltpu.make_async_remote_copy(
            src_ref=source,
            dst_ref=target,
            send_sem=send_sem.at[base + k],
            recv_sem=recv_sem.at[base + k],
            device_id=device,
            device_id_type=MESH,
        )

    hops = [
        describe(h, o_ref.at[pl.ds(h * half, half)], hop.at[h], z_dev[1 + h]) for h in range(2)
    ]
    ends = [
        describe(2 + h, o_ref.at[pl.ds((1 + h) * tiles, tiles)], got.at[1 - h], z_dev[1 + h])
        for h in range(2)
    ]
    last = [
        describe(4 + h, hop.at[h], got.at[2, pl.ds(h * half, half)], z_dev[1 + h]) for h in range(2)
    ]

    scores(jnp.int32(0), 0)
    scores(jnp.int32(1), 1)
    weights(0)

    def pair(k, carry):
        for r in range(2):
            n = 2 * k + r
            values(n, r)
            scores(n + 2, r)
            weights(1 - r)

        @pl.when(k == 2)
        def _():
            for c in hops:
                c.start()

        @pl.when(k == 4)
        def _():
            ends[0].start()

        @pl.when(k == 5)
        def _():
            for c, d in zip(hops, last):
                c.wait_recv()
                d.start()

        @pl.when(k == 6)
        def _():
            ends[1].start()

        return carry

    lax.fori_loop(0, count // 2 - 1, pair, 0)
    values(jnp.int32(count - 2), 0)
    weights(1)
    values(jnp.int32(count - 1), 1)

    def add_head(pz, piece):
        o = piece.reshape(tiles * TILE, HD)
        w = wo_ref[pl.ds(pl.multiple_of(pz * HD, HD), HD), :]
        return jnp.dot(o, w, preferred_element_type=jnp.float32)

    for c in loads[7:]:
        c.wait()
    res_ref[...] = x_ref[...].astype(jnp.float32) + add_head(z, o_ref[3 * tiles:])
    for c in last:
        c.wait_recv()
    res_ref[...] += add_head(z_at[3], got[2])
    for h in (1, 0):
        ends[1 - h].wait_recv()
        res_ref[...] += add_head(z_at[1 + h], got[h])
    r = res_ref[...]
    inverse = lax.rsqrt(jnp.mean(r * r, axis=-1, keepdims=True) + 1e-06)
    norm_ref[...] = (r * inverse).astype(jnp.bfloat16)
    width = 256

    def hidden(f, carry):
        cols = pl.ds(pl.multiple_of(f * width, width), width)
        gate = jnp.dot(norm_ref[...], wg_ref[:, cols], preferred_element_type=jnp.float32)
        lift = jnp.dot(norm_ref[...], wu_ref[:, cols], preferred_element_type=jnp.float32)
        hid_ref[:, cols] = (gate / (1.0 + jnp.exp(-gate)) * lift).astype(jnp.bfloat16)
        return carry

    lax.fori_loop(0, wg_ref.shape[1] // width, hidden, 0)

    def lower(f, carry):
        cols = pl.ds(pl.multiple_of(f * width, width), width)
        out_ref[:, cols] = (
            res_ref[:, cols]
            + jnp.dot(hid_ref[...], wd_ref[:, cols], preferred_element_type=jnp.float32)
        ).astype(jnp.bfloat16)
        return carry

    lax.fori_loop(0, D // width, lower, 0)
    for c in live + hops + ends + last:
        c.wait_send()


def body(
    x, lists, counts, valid, w_query, w_key, w_value, w_out, w_gate, w_up, w_down
):
    tiles = x.shape[0] // TILE
    piece = (tiles, 2, TILE, HD)
    weights = (w_query, w_key, w_value, w_out, w_gate, w_up, w_down)
    copied = (x,) + weights

    def fast(shape, dtype=x.dtype):
        return pltpu.VMEM(shape, dtype)

    return pl.pallas_call(
        layer_kernel,
        out_shape=jax.ShapeDtypeStruct(x.shape, x.dtype),
        in_specs=[pl.BlockSpec(memory_space=pltpu.HBM)] * 11,
        out_specs=pl.BlockSpec(memory_space=pltpu.VMEM),
        scratch_shapes=[
            fast(lists.shape, jnp.int32),
            pltpu.SMEM(counts.shape, jnp.int32),
            pltpu.SMEM(valid.shape, jnp.int32),
        ]
        + [fast(a.shape) for a in copied]
        + [
            fast((6 * 2 * ZD * tiles,) + piece[1:]),
            fast((ZD, tiles, TILE, HD)),
            fast((HEADS,) + piece),
            fast((HEADS, tiles, TILE, HD)),
            fast((8, 128), jnp.int32),
            fast((ZD, 8, 128), jnp.int32),
            fast((PARTS, tiles // PARTS) + piece[1:]),
            fast((len(DIRECT), tiles // PARTS) + piece[1:]),
            fast((ZD * tiles, 128), jnp.int32),
            pltpu.SMEM((ZD * tiles, 128), jnp.int32),
        ]
        + [fast((TILE, NB * TILE), jnp.float32)] * 2
        + [fast((TILE, NB * TILE))] * 2
        + [fast((TILE, TILE), jnp.float32)] * 4
        + [
            fast((ZD * tiles, TILE, HD)),
            fast((ZD - 1, tiles, TILE, HD)),
            fast((2, tiles // 2, TILE, HD)),
            fast(x.shape, jnp.float32),
            fast(x.shape),
            fast((x.shape[0], w_gate.shape[1])),
            pltpu.SemaphoreType.DMA((12,)),
            pltpu.SemaphoreType.DMA((COPIES,)),
            pltpu.SemaphoreType.DMA((COPIES,)),
        ],
        compiler_params=pltpu.CompilerParams(
            collective_id=0, has_side_effects=True, vmem_limit_bytes=67043328
        ),
    )(lists, counts, valid, x, *weights)


def solution(mesh):
    placed = (
        P(("zone", "dev"), None),
        P(("zone", "dev"), None),
        P(("zone", "dev")),
        P(),
        P(),
        P(),
        P(),
        P(),
        P(),
        P(),
        P(),
    )
    return jax.shard_map(
        body, mesh=mesh, in_specs=placed, out_specs=P(("zone", "dev"), None), check_vma=False
    )
```

```python
import heapq
import math

import jax
import jax.numpy as jnp
from jax import lax
from jax.experimental import pallas as pl
from jax.experimental.pallas import tpu as pltpu
from jax.sharding import PartitionSpec as P

D = 512
HEADS = 4
HD = 128
TILE = 128
NB = 32
ZD = 4
NEG = -1e30
EXP_SCALE = math.log2(math.e) / math.sqrt(HD)


MESH = pl.DeviceIdType.MESH
PARTS = 4
DIRECT = ((1, 0), (1, 1), (1, 2), (1, 3), (2, 0), (2, 2))
OPENING = (("own", 0), ("next", 1), ("next", 3), ("relay", 1), ("next", 2), ("relay", 2), ("own", 3), ("own", 2), ("next", 0), ("relay", 3), ("own", 1), ("relay", 0))
FAR_UP = ((0, 0), (1, 0), (1, 2), (2, 0), (2, 3), (3, 0), (3, 1), (3, 3))


COPIES = 210


def arrivals():
    unit, hop = 5.6 / PARTS, 3.1
    free, events, order = {}, [], []

    def send(now, key, link):
        free[link] = max(now, free.get(link, 0.0)) + unit
        heapq.heappush(events, (free[link] + hop, len(order) + len(events), key))

    def own(now, u):
        if u in DIRECT:
            send(now, ("transit", u), "back")
        else:
            send(now, ("below", u), "up")
            send(now, ("above", u), "down")

    for kind, h in OPENING:
        if kind == "own":
            own(0.0, (0, h))
        elif kind == "next":
            send(0.0, ("own", (2, h)), "next")
            send(0.0, ("own", (1, h)), "prior")
        else:
            send(0.0, ("relay", h), "next" if 2 * h < PARTS else "prior")
    while events:
        now, _, (kind, u) = heapq.heappop(events)
        order.append((kind, u))
        if kind == "own":
            own(now, u)
        elif kind == "relay":
            send(now, ("own", (3, u)), "next" if 2 * u < PARTS else "prior")
        elif kind == "transit":
            send(now, ("halo_below", u), "up")
            send(now, ("halo_above", u), "down")
        elif kind in ("above", "below"):
            if (kind == "below") == (u in FAR_UP):
                send(now, ("far", u), "up" if kind == "below" else "down")
            if u not in DIRECT:
                send(now, ("halo_" + kind, u), "halo")
        elif kind in ("halo_above", "halo_below") and u in DIRECT:
            send(now, (kind[5:], u), "back")
    return order


def layer_kernel(
    nb_hbm, count_hbm, valid_hbm, x_hbm, wq_hbm, wk_hbm, wv_hbm, wo_hbm, wg_hbm, wu_hbm, wd_hbm,
    out_ref,
    nb_ref, count_ref, valid_ref, x_ref, wq_ref, wk_ref, wv_ref, wo_ref, wg_ref, wu_ref, wd_ref,
    kv_out, q_out, kv_ref, q_ref, raw, raw_all, relay, transit, code_vec, code_ref,
    s_even, s_odd, p_even, p_odd, t_even, t_odd,
    o_ref, got, hop, res_ref, norm_ref, hid_ref,
    load_sem, send_sem, recv_sem,
):
    zone, dev = lax.axis_index("zone"), lax.axis_index("dev")
    x, y_lo = zone // 2, zone % 2
    y_hi, z, core = dev // 8, (dev // 2) % ZD, dev % 2
    y = y_hi * 2 + y_lo
    tiles = x_ref.shape[0] // TILE
    size = tiles // PARTS
    half = tiles // 2

    def at(px, py, pz, pc):
        return (px * 2 + py % 2, (py // 2) * 8 + pz * 2 + pc)

    side = 1 - 2 * y_lo
    up, down = at(x, (y + 1) % 4, z, core), at(x, (y + 3) % 4, z, core)
    halo, back = at((x + 4 + side) % 4, y, z, core), at((x + 4 - side) % 4, y, z, core)
    partner = at(x, y, z, 1 - core)
    z_at = [(z + d) % ZD for d in (0, 1, 3, 2)]
    z_dev = [at(x, y, pz, core) for pz in z_at]

    barrier = pltpu.get_barrier_semaphore()
    peers = [up, down, halo, back, partner] + z_dev[1:]
    for peer in peers:
        pl.semaphore_signal(barrier, inc=1, device_id=peer, device_id_type=MESH)

    loads = [
        pltpu.make_async_copy(source, target, load_sem.at[i])
        for i, (source, target) in enumerate(
            (
                (x_hbm, x_ref), (wk_hbm, wk_ref), (wv_hbm, wv_ref), (nb_hbm, nb_ref),
                (count_hbm, count_ref), (wq_hbm, wq_ref), (valid_hbm, valid_ref),
                (wo_hbm, wo_ref), (wg_hbm, wg_ref), (wu_hbm, wu_ref), (wd_hbm, wd_ref),
            )
        )
    ]
    for c in loads:
        c.start()
    for c in loads[:5]:
        c.wait()

    lane = lax.broadcasted_iota(jnp.int32, (1, 128), 1)
    raw[...] = jnp.full(raw.shape, -1, jnp.int32)
    raw[:tiles, :NB] = nb_ref[...]
    for t in range(tiles):
        n = count_ref[t]
        row = jnp.where(lane < jnp.minimum(n, NB), raw[t:t + 1, :], -1)
        raw[t:t + 1, :] = jnp.where(lane == NB, n, row)

    def rows_of(t):
        return x_ref[pl.ds(pl.multiple_of(t * TILE, TILE), TILE), :]

    def keys_values(t, carry):
        rows = rows_of(t)
        k = jnp.dot(rows, wk_ref[...], preferred_element_type=jnp.float32)
        for h in range(HEADS):
            kv_ref[h, t, 0] = jnp.transpose(k[:, h * HD:(h + 1) * HD]).astype(jnp.bfloat16)
        v = jnp.dot(rows, wv_ref[...], preferred_element_type=jnp.float32).astype(jnp.bfloat16)
        for h in range(HEADS):
            kv_ref[h, t, 1] = v[:, h * HD:(h + 1) * HD]
        return carry

    lax.fori_loop(0, tiles, keys_values, 0)
    kv_out[pl.ds((core * ZD + z) * tiles, tiles)] = kv_ref[z]
    pl.semaphore_wait(barrier, len(peers))

    live, flying, shared = [], {}, []

    def send(source, target, device):
        k = len(live)
        copy = pltpu.make_async_remote_copy(
            src_ref=source,
            dst_ref=target,
            send_sem=send_sem.at[k],
            recv_sem=recv_sem.at[k],
            device_id=device,
            device_id_type=MESH,
        )
        copy.start()
        live.append(copy)
        return copy

    def part(h):
        return pl.ds(h * size, size)

    def spot_of(slot, pz, h):
        return kv_out.at[pl.ds(((slot * 2 + core) * ZD + pz) * tiles + h * size, size)]

    def place(slot, u):
        return spot_of(slot, z_at[u[0]], u[1])

    def share(slot, u, source=None):
        shared.append(send(place(slot, u) if source is None else source, place(slot, u), partner))

    def own(u, source):
        if u in DIRECT:
            flying["transit", u] = send(source, transit.at[DIRECT.index(u)], back)
        else:
            flying["below", u] = send(source, place(2, u), up)
            flying["above", u] = send(source, place(1, u), down)
        share(0, u, source)

    def forward(kind, u):
        flying[kind, u].wait_recv()
        if kind == "own":
            own(u, place(0, u))
        elif kind == "relay":
            along = 2 * u < PARTS
            flying["own", (3, u)] = send(
                relay.at[u], spot_of(0, z_at[2 if along else 1], u), z_dev[1 if along else 2]
            )
        elif kind == "transit":
            spot = transit.at[DIRECT.index(u)]
            flying["halo_below", u] = send(spot, place(5, u), up)
            flying["halo_above", u] = send(spot, place(4, u), down)
        elif kind in ("above", "below"):
            slot = 1 if kind == "above" else 2
            if (kind == "below") == (u in FAR_UP):
                flying["far", u] = send(
                    place(slot, u), place(3, u), up if kind == "below" else down
                )
            if u not in DIRECT:
                flying["halo_" + kind, u] = send(place(slot, u), place(slot + 3, u), halo)
            share(slot, u)
        elif kind == "far":
            share(3, u)
        else:
            slot = 4 if kind == "halo_above" else 5
            if u in DIRECT:
                flying[kind[5:], u] = send(place(slot, u), place(slot - 3, u), back)
            share(slot, u)

    for kind, h in OPENING:
        if kind == "own":
            own((0, h), kv_ref.at[z, part(h)])
        elif kind == "next":
            flying["own", (2, h)] = send(
                kv_ref.at[z_at[1], part(h)], spot_of(0, z, h), z_dev[1]
            )
            flying["own", (1, h)] = send(
                kv_ref.at[z_at[2], part(h)], spot_of(0, z, h), z_dev[2]
            )
        else:
            flying["relay", h] = send(
                kv_ref.at[z_at[3], part(h)], relay.at[h], z_dev[1 if 2 * h < PARTS else 2]
            )

    def queries(t, carry):
        q = jnp.dot(rows_of(t), wq_ref[...], preferred_element_type=jnp.float32)
        q = q.astype(jnp.bfloat16)
        for h in range(HEADS):
            q_ref[h, t] = q[:, h * HD:(h + 1) * HD]
        return carry

    loads[5].wait()
    lax.fori_loop(0, tiles, queries, 0)
    q_out[z] = q_ref[z]
    raw_all[z] = raw[...]

    order = arrivals()
    relays = [n for n, (kind, _) in enumerate(order) if kind == "relay"]
    middle = 2 * len(order) // 3
    for kind, u in order[:relays[-1] + 1]:
        forward(kind, u)
    q_in, raw_in = {}, {}
    for j, lands in ((1, 2), (2, 1), (3, 3)):
        raw_in[lands] = send(raw, raw_all.at[z], z_dev[j])
        q_in[lands] = send(q_ref.at[z_at[j]], q_out.at[z], z_dev[j])
    for kind, u in order[relays[-1] + 1:middle]:
        forward(kind, u)

    for j in (1, 2, 3):
        raw_in[j].wait_recv()
    lists = raw_all[...].reshape(ZD * raw.shape[0], 128)

    loads[6].wait()

    span = 3 * 64

    def look_up(i, found):
        g = (zone * 64 + valid_ref.shape[0] - 64 + i) % valid_ref.shape[0]
        return jnp.where(lists == g, valid_ref[g], found)

    found = lax.fori_loop(0, span, look_up, jnp.zeros_like(lists), unroll=8)
    spot = jnp.maximum(lists, 0)
    relative = (spot // 64 + 9 - zone) % 8
    there_y = (spot // 32) % 2 * 2 + 1 - y_lo
    near = jnp.where((there_y + 4 - y) % 4 == 1, 1, 2)
    near = near + jnp.where(relative == 2 - 2 * y_lo, 0, 3)
    slot = jnp.where(relative == 1, jnp.where((spot // 32) % 2 == y_hi, 0, 3), near)
    code = ((slot * 2 + (spot // 4) % 2) * ZD + (spot // 8) % ZD) * 4 + spot % 4
    code = jnp.where(lists < 0, 0, code * 256 + found)
    code = jnp.where(lane == NB, lists, code)
    for p in range(ZD):
        code_vec[p * tiles:(p + 1) * tiles, :] = code[p * raw.shape[0]:p * raw.shape[0] + tiles]

    to_smem = pltpu.make_async_copy(code_vec, code_ref, load_sem.at[11])
    to_smem.start()
    for kind, u in order[middle:]:
        forward(kind, u)
    for c in shared + list(q_in.values()):
        c.wait_recv()
    to_smem.wait()

    s_bufs, p_bufs = (s_even, s_odd), (p_even, p_odd)
    t_bufs = (t_even, t_odd)
    count = ZD * tiles

    def owner(n):
        g = n // tiles
        d = jnp.where(g == 0, 2, jnp.where(g == 1, 1, jnp.where(g == 2, 3, 0)))
        return (z + d) % ZD

    def scores(n, b):
        pz, t = owner(n), n % tiles
        i = pz * tiles + t
        q = q_out[pz, t]
        top = None
        for p in range(NB // 2):
            e, f = code_ref[i, 2 * p], code_ref[i, 2 * p + 1]
            keys = jnp.concatenate([kv_out[e // 256, 0], kv_out[f // 256, 0]], axis=1)
            s = jnp.dot(q, keys, preferred_element_type=jnp.float32)
            bias = jnp.concatenate(
                [jnp.where(lane < e % 256, 0.0, NEG), jnp.where(lane < f % 256, 0.0, NEG)],
                axis=1,
            )
            s = s + bias
            s_bufs[b][:, p * 256:(p + 1) * 256] = s
            pair_top = jnp.maximum(s[:, :TILE], s[:, TILE:])
            top = pair_top if top is None else jnp.maximum(top, pair_top)
        t_bufs[b][...] = top

    def weights(b):
        for g in range(TILE // 16):
            rows = slice(g * 16, (g + 1) * 16)
            peak = jnp.max(t_bufs[b][rows, :], axis=1, keepdims=True)
            for k in range(NB):
                cols = slice(k * TILE, (k + 1) * TILE)
                w = jnp.exp2((s_bufs[b][rows, cols] - peak) * EXP_SCALE)
                p_bufs[b][rows, cols] = w.astype(jnp.bfloat16)

    def values(n, b):
        i = owner(n) * tiles + n % tiles
        ones = jnp.ones((2 * TILE, TILE), jnp.bfloat16)
        acc = None
        for p in range(NB // 2):
            e, f = code_ref[i, 2 * p], code_ref[i, 2 * p + 1]
            v = jnp.concatenate([kv_out[e // 256, 1], kv_out[f // 256, 1]], axis=0)
            share_p = jnp.dot(
                p_bufs[b][:, p * 256:(p + 1) * 256],
                jnp.concatenate([v, ones], axis=1),
                preferred_element_type=jnp.float32,
            )
            acc = share_p if acc is None else acc + share_p
        o_ref[n] = (acc[:, :HD] / acc[:, HD:]).astype(jnp.bfloat16)

    base = len(live)

    def describe(k, source, target, device):
        return pltpu.make_async_remote_copy(
            src_ref=source,
            dst_ref=target,
            send_sem=send_sem.at[base + k],
            recv_sem=recv_sem.at[base + k],
            device_id=device,
            device_id_type=MESH,
        )

    hops = [
        describe(h, o_ref.at[pl.ds(h * half, half)], hop.at[h], z_dev[1 + h]) for h in range(2)
    ]
    ends = [
        describe(2 + h, o_ref.at[pl.ds((1 + h) * tiles, tiles)], got.at[1 - h], z_dev[1 + h])
        for h in range(2)
    ]
    last = [
        describe(4 + h, hop.at[h], got.at[2, pl.ds(h * half, half)], z_dev[1 + h]) for h in range(2)
    ]

    scores(jnp.int32(0), 0)
    scores(jnp.int32(1), 1)
    weights(0)

    def pair(k, carry):
        for r in range(2):
            n = 2 * k + r
            values(n, r)
            scores(n + 2, r)
            weights(1 - r)

        @pl.when(k == 2)
        def _():
            for c in hops:
                c.start()

        @pl.when(k == 4)
        def _():
            ends[0].start()

        @pl.when(k == 5)
        def _():
            for c, d in zip(hops, last):
                c.wait_recv()
                d.start()

        @pl.when(k == 6)
        def _():
            ends[1].start()

        return carry

    lax.fori_loop(0, count // 2 - 1, pair, 0)
    values(jnp.int32(count - 2), 0)
    weights(1)
    values(jnp.int32(count - 1), 1)

    def add_head(pz, piece):
        o = piece.reshape(tiles * TILE, HD)
        w = wo_ref[pl.ds(pl.multiple_of(pz * HD, HD), HD), :]
        return jnp.dot(o, w, preferred_element_type=jnp.float32)

    for c in loads[7:]:
        c.wait()
    res_ref[...] = x_ref[...].astype(jnp.float32) + add_head(z, o_ref[3 * tiles:])
    for c in last:
        c.wait_recv()
    res_ref[...] += add_head(z_at[3], got[2])
    for h in (1, 0):
        ends[1 - h].wait_recv()
        res_ref[...] += add_head(z_at[1 + h], got[h])
    r = res_ref[...]
    inverse = lax.rsqrt(jnp.mean(r * r, axis=-1, keepdims=True) + 1e-06)
    norm_ref[...] = (r * inverse).astype(jnp.bfloat16)
    width = 256
    broad = 512

    def hidden(f, carry):
        cols = pl.ds(pl.multiple_of(f * broad, broad), broad)
        gate = jnp.dot(norm_ref[...], wg_ref[:, cols], preferred_element_type=jnp.float32)
        lift = jnp.dot(norm_ref[...], wu_ref[:, cols], preferred_element_type=jnp.float32)
        hid_ref[:, cols] = (gate / (1.0 + jnp.exp(-gate)) * lift).astype(jnp.bfloat16)
        return carry

    lax.fori_loop(0, wg_ref.shape[1] // broad, hidden, 0)

    def lower(f, carry):
        cols = pl.ds(pl.multiple_of(f * width, width), width)
        out_ref[:, cols] = (
            res_ref[:, cols]
            + jnp.dot(hid_ref[...], wd_ref[:, cols], preferred_element_type=jnp.float32)
        ).astype(jnp.bfloat16)
        return carry

    lax.fori_loop(0, D // width, lower, 0)
    for c in live + hops + ends + last:
        c.wait_send()


def body(
    x, lists, counts, valid, w_query, w_key, w_value, w_out, w_gate, w_up, w_down
):
    tiles = x.shape[0] // TILE
    piece = (tiles, 2, TILE, HD)
    weights = (w_query, w_key, w_value, w_out, w_gate, w_up, w_down)
    copied = (x,) + weights

    def fast(shape, dtype=x.dtype):
        return pltpu.VMEM(shape, dtype)

    return pl.pallas_call(
        layer_kernel,
        out_shape=jax.ShapeDtypeStruct(x.shape, x.dtype),
        in_specs=[pl.BlockSpec(memory_space=pltpu.HBM)] * 11,
        out_specs=pl.BlockSpec(memory_space=pltpu.VMEM),
        scratch_shapes=[
            fast(lists.shape, jnp.int32),
            pltpu.SMEM(counts.shape, jnp.int32),
            pltpu.SMEM(valid.shape, jnp.int32),
        ]
        + [fast(a.shape) for a in copied]
        + [
            fast((6 * 2 * ZD * tiles,) + piece[1:]),
            fast((ZD, tiles, TILE, HD)),
            fast((HEADS,) + piece),
            fast((HEADS, tiles, TILE, HD)),
            fast((8, 128), jnp.int32),
            fast((ZD, 8, 128), jnp.int32),
            fast((PARTS, tiles // PARTS) + piece[1:]),
            fast((len(DIRECT), tiles // PARTS) + piece[1:]),
            fast((ZD * tiles, 128), jnp.int32),
            pltpu.SMEM((ZD * tiles, 128), jnp.int32),
        ]
        + [fast((TILE, NB * TILE), jnp.float32)] * 2
        + [fast((TILE, NB * TILE))] * 2
        + [fast((TILE, TILE), jnp.float32)] * 2
        + [
            fast((ZD * tiles, TILE, HD)),
            fast((ZD - 1, tiles, TILE, HD)),
            fast((2, tiles // 2, TILE, HD)),
            fast(x.shape, jnp.float32),
            fast(x.shape),
            fast((x.shape[0], w_gate.shape[1])),
            pltpu.SemaphoreType.DMA((12,)),
            pltpu.SemaphoreType.DMA((COPIES,)),
            pltpu.SemaphoreType.DMA((COPIES,)),
        ],
        compiler_params=pltpu.CompilerParams(
            collective_id=0, has_side_effects=True, vmem_limit_bytes=67043328
        ),
    )(lists, counts, valid, x, *weights)


def solution(mesh):
    placed = (
        P(("zone", "dev"), None),
        P(("zone", "dev"), None),
        P(("zone", "dev")),
        P(),
        P(),
        P(),
        P(),
        P(),
        P(),
        P(),
        P(),
    )
    return jax.shard_map(
        body, mesh=mesh, in_specs=placed, out_specs=P(("zone", "dev"), None), check_vma=False
    )
```

```python
import heapq
import math

import jax
import jax.numpy as jnp
from jax import lax
from jax.experimental import pallas as pl
from jax.experimental.pallas import tpu as pltpu
from jax.sharding import PartitionSpec as P

D = 512
HEADS = 4
HD = 128
TILE = 128
NB = 32
ZD = 4
NEG = -1e30
EXP_SCALE = math.log2(math.e) / math.sqrt(HD)


MESH = pl.DeviceIdType.MESH
PARTS = 4
DIRECT = ((1, 0), (1, 1), (1, 2), (1, 3), (2, 0), (2, 2))
OPENING = (("own", 0), ("next", 1), ("next", 3), ("relay", 1), ("next", 2), ("relay", 2), ("own", 3), ("own", 2), ("next", 0), ("relay", 3), ("own", 1), ("relay", 0))
FAR_UP = ((0, 0), (1, 0), (1, 2), (2, 0), (2, 3), (3, 0), (3, 1), (3, 3))


COPIES = 210


def arrivals():
    unit, hop = 5.6 / PARTS, 3.1
    free, events, order = {}, [], []

    def send(now, key, link):
        free[link] = max(now, free.get(link, 0.0)) + unit
        heapq.heappush(events, (free[link] + hop, len(order) + len(events), key))

    def own(now, u):
        if u in DIRECT:
            send(now, ("transit", u), "back")
        else:
            send(now, ("below", u), "up")
            send(now, ("above", u), "down")

    for kind, h in OPENING:
        if kind == "own":
            own(0.0, (0, h))
        elif kind == "next":
            send(0.0, ("own", (2, h)), "next")
            send(0.0, ("own", (1, h)), "prior")
        else:
            send(0.0, ("relay", h), "next" if 2 * h < PARTS else "prior")
    while events:
        now, _, (kind, u) = heapq.heappop(events)
        order.append((kind, u))
        if kind == "own":
            own(now, u)
        elif kind == "relay":
            send(now, ("own", (3, u)), "next" if 2 * u < PARTS else "prior")
        elif kind == "transit":
            send(now, ("halo_below", u), "up")
            send(now, ("halo_above", u), "down")
        elif kind in ("above", "below"):
            if (kind == "below") == (u in FAR_UP):
                send(now, ("far", u), "up" if kind == "below" else "down")
            if u not in DIRECT:
                send(now, ("halo_" + kind, u), "halo")
        elif kind in ("halo_above", "halo_below") and u in DIRECT:
            send(now, (kind[5:], u), "back")
    return order


def layer_kernel(
    nb_hbm, count_hbm, valid_hbm, x_hbm, wq_hbm, wk_hbm, wv_hbm, wo_hbm, wg_hbm, wu_hbm, wd_hbm,
    out_ref,
    nb_ref, count_ref, valid_ref, x_ref, wq_ref, wk_ref, wv_ref, wo_ref, wg_ref, wu_ref, wd_ref,
    kv_out, q_out, kv_ref, q_ref, raw, raw_all, relay, transit, code_vec, code_ref,
    s_even, s_odd, p_even, p_odd, t_even, t_odd,
    o_ref, seen, got, hop, res_ref, norm_ref, hid_ref,
    load_sem, send_sem, recv_sem,
):
    zone, dev = lax.axis_index("zone"), lax.axis_index("dev")
    x, y_lo = zone // 2, zone % 2
    y_hi, z, core = dev // 8, (dev // 2) % ZD, dev % 2
    y = y_hi * 2 + y_lo
    tiles = x_ref.shape[0] // TILE
    size = tiles // PARTS
    half = tiles // 2

    def at(px, py, pz, pc):
        return (px * 2 + py % 2, (py // 2) * 8 + pz * 2 + pc)

    side = 1 - 2 * y_lo
    up, down = at(x, (y + 1) % 4, z, core), at(x, (y + 3) % 4, z, core)
    halo, back = at((x + 4 + side) % 4, y, z, core), at((x + 4 - side) % 4, y, z, core)
    partner = at(x, y, z, 1 - core)
    z_at = [(z + d) % ZD for d in (0, 1, 3, 2)]
    z_dev = [at(x, y, pz, core) for pz in z_at]

    barrier = pltpu.get_barrier_semaphore()
    peers = [up, down, halo, back, partner] + z_dev[1:]
    for peer in peers:
        pl.semaphore_signal(barrier, inc=1, device_id=peer, device_id_type=MESH)

    loads = [
        pltpu.make_async_copy(source, target, load_sem.at[i])
        for i, (source, target) in enumerate(
            (
                (x_hbm, x_ref), (wk_hbm, wk_ref), (wv_hbm, wv_ref), (nb_hbm, nb_ref),
                (count_hbm, count_ref), (wq_hbm, wq_ref), (valid_hbm, valid_ref),
                (wo_hbm, wo_ref), (wg_hbm, wg_ref), (wu_hbm, wu_ref), (wd_hbm, wd_ref),
            )
        )
    ]
    for c in loads:
        c.start()
    for c in loads[:5]:
        c.wait()

    lane = lax.broadcasted_iota(jnp.int32, (1, 128), 1)
    raw[...] = jnp.full(raw.shape, -1, jnp.int32)
    raw[:tiles, :NB] = nb_ref[...]
    for t in range(tiles):
        n = count_ref[t]
        row = jnp.where(lane < jnp.minimum(n, NB), raw[t:t + 1, :], -1)
        raw[t:t + 1, :] = jnp.where(lane == NB, n, row)

    def rows_of(t):
        return x_ref[pl.ds(pl.multiple_of(t * TILE, TILE), TILE), :]

    def keys_values(t, carry):
        rows = rows_of(t)
        k = jnp.dot(rows, wk_ref[...], preferred_element_type=jnp.float32)
        for h in range(HEADS):
            kv_ref[h, t, 0] = jnp.transpose(k[:, h * HD:(h + 1) * HD]).astype(jnp.bfloat16)
        v = jnp.dot(rows, wv_ref[...], preferred_element_type=jnp.float32).astype(jnp.bfloat16)
        for h in range(HEADS):
            kv_ref[h, t, 1] = v[:, h * HD:(h + 1) * HD]
        return carry

    lax.fori_loop(0, tiles, keys_values, 0)
    kv_out[pl.ds((core * ZD + z) * tiles, tiles)] = kv_ref[z]
    pl.semaphore_wait(barrier, len(peers))

    live, flying, shared = [], {}, []

    def send(source, target, device):
        k = len(live)
        copy = pltpu.make_async_remote_copy(
            src_ref=source,
            dst_ref=target,
            send_sem=send_sem.at[k],
            recv_sem=recv_sem.at[k],
            device_id=device,
            device_id_type=MESH,
        )
        copy.start()
        live.append(copy)
        return copy

    def part(h):
        return pl.ds(h * size, size)

    def spot_of(slot, pz, h):
        return kv_out.at[pl.ds(((slot * 2 + core) * ZD + pz) * tiles + h * size, size)]

    def place(slot, u):
        return spot_of(slot, z_at[u[0]], u[1])

    def share(slot, u, source=None):
        shared.append(send(place(slot, u) if source is None else source, place(slot, u), partner))

    def own(u, source):
        if u in DIRECT:
            flying["transit", u] = send(source, transit.at[DIRECT.index(u)], back)
        else:
            flying["below", u] = send(source, place(2, u), up)
            flying["above", u] = send(source, place(1, u), down)
        share(0, u, source)

    def forward(kind, u):
        flying[kind, u].wait_recv()
        if kind == "own":
            own(u, place(0, u))
        elif kind == "relay":
            along = 2 * u < PARTS
            flying["own", (3, u)] = send(
                relay.at[u], spot_of(0, z_at[2 if along else 1], u), z_dev[1 if along else 2]
            )
        elif kind == "transit":
            spot = transit.at[DIRECT.index(u)]
            flying["halo_below", u] = send(spot, place(5, u), up)
            flying["halo_above", u] = send(spot, place(4, u), down)
        elif kind in ("above", "below"):
            slot = 1 if kind == "above" else 2
            if (kind == "below") == (u in FAR_UP):
                flying["far", u] = send(
                    place(slot, u), place(3, u), up if kind == "below" else down
                )
            if u not in DIRECT:
                flying["halo_" + kind, u] = send(place(slot, u), place(slot + 3, u), halo)
            share(slot, u)
        elif kind == "far":
            share(3, u)
        else:
            slot = 4 if kind == "halo_above" else 5
            if u in DIRECT:
                flying[kind[5:], u] = send(place(slot, u), place(slot - 3, u), back)
            share(slot, u)

    for kind, h in OPENING:
        if kind == "own":
            own((0, h), kv_ref.at[z, part(h)])
        elif kind == "next":
            flying["own", (2, h)] = send(
                kv_ref.at[z_at[1], part(h)], spot_of(0, z, h), z_dev[1]
            )
            flying["own", (1, h)] = send(
                kv_ref.at[z_at[2], part(h)], spot_of(0, z, h), z_dev[2]
            )
        else:
            flying["relay", h] = send(
                kv_ref.at[z_at[3], part(h)], relay.at[h], z_dev[1 if 2 * h < PARTS else 2]
            )

    def queries(t, carry):
        q = jnp.dot(rows_of(t), wq_ref[...], preferred_element_type=jnp.float32)
        q = q.astype(jnp.bfloat16)
        for h in range(HEADS):
            q_ref[h, t] = q[:, h * HD:(h + 1) * HD]
        return carry

    loads[5].wait()
    lax.fori_loop(0, tiles, queries, 0)
    q_out[z] = q_ref[z]
    raw_all[z] = raw[...]

    order = arrivals()
    relays = [n for n, (kind, _) in enumerate(order) if kind == "relay"]
    middle = 2 * len(order) // 3
    for kind, u in order[:relays[-1] + 1]:
        forward(kind, u)
    q_in, raw_in = {}, {}
    for j, lands in ((1, 2), (2, 1), (3, 3)):
        raw_in[lands] = send(raw, raw_all.at[z], z_dev[j])
        q_in[lands] = send(q_ref.at[z_at[j]], q_out.at[z], z_dev[j])
    for kind, u in order[relays[-1] + 1:middle]:
        forward(kind, u)

    for j in (1, 2, 3):
        raw_in[j].wait_recv()
    lists = raw_all[...].reshape(ZD * raw.shape[0], 128)

    loads[6].wait()

    span = 3 * 64

    def look_up(i, found):
        g = (zone * 64 + valid_ref.shape[0] - 64 + i) % valid_ref.shape[0]
        return jnp.where(lists == g, valid_ref[g], found)

    found = lax.fori_loop(0, span, look_up, jnp.zeros_like(lists), unroll=8)
    spot = jnp.maximum(lists, 0)
    relative = (spot // 64 + 9 - zone) % 8
    there_y = (spot // 32) % 2 * 2 + 1 - y_lo
    near = jnp.where((there_y + 4 - y) % 4 == 1, 1, 2)
    near = near + jnp.where(relative == 2 - 2 * y_lo, 0, 3)
    slot = jnp.where(relative == 1, jnp.where((spot // 32) % 2 == y_hi, 0, 3), near)
    code = ((slot * 2 + (spot // 4) % 2) * ZD + (spot // 8) % ZD) * 4 + spot % 4
    code = jnp.where(lists < 0, 0, code * 256 + found)
    code = jnp.where(lane == NB, lists, code)
    for p in range(ZD):
        code_vec[p * tiles:(p + 1) * tiles, :] = code[p * raw.shape[0]:p * raw.shape[0] + tiles]

    to_smem = pltpu.make_async_copy(code_vec, code_ref, load_sem.at[11])
    to_smem.start()
    for kind, u in order[middle:]:
        forward(kind, u)
    for c in shared + list(q_in.values()):
        c.wait_recv()
    to_smem.wait()

    s_bufs, p_bufs = (s_even, s_odd), (p_even, p_odd)
    t_bufs = (t_even, t_odd)
    count = ZD * tiles

    def owner(n):
        g = n // tiles
        d = jnp.where(g == 0, 2, jnp.where(g == 1, 1, jnp.where(g == 2, 3, 0)))
        return (z + d) % ZD

    def scores(n, b):
        pz, t = owner(n), n % tiles
        i = pz * tiles + t
        q = q_out[pz, t]
        top = None
        for p in range(NB // 2):
            e, f = code_ref[i, 2 * p], code_ref[i, 2 * p + 1]
            keys = jnp.concatenate([kv_out[e // 256, 0], kv_out[f // 256, 0]], axis=1)
            s = jnp.dot(q, keys, preferred_element_type=jnp.float32)
            bias = jnp.concatenate(
                [jnp.where(lane < e % 256, 0.0, NEG), jnp.where(lane < f % 256, 0.0, NEG)],
                axis=1,
            )
            s = s + bias
            s_bufs[b][:, p * 256:(p + 1) * 256] = s
            pair_top = jnp.maximum(s[:, :TILE], s[:, TILE:])
            top = pair_top if top is None else jnp.maximum(top, pair_top)
        t_bufs[b][...] = top

    def weights(b):
        for g in range(TILE // 16):
            rows = slice(g * 16, (g + 1) * 16)
            peak = jnp.max(t_bufs[b][rows, :], axis=1, keepdims=True)
            for k in range(NB):
                cols = slice(k * TILE, (k + 1) * TILE)
                w = jnp.exp2((s_bufs[b][rows, cols] - peak) * EXP_SCALE)
                p_bufs[b][rows, cols] = w.astype(jnp.bfloat16)

    def values(n, b):
        i = owner(n) * tiles + n % tiles
        ones = jnp.ones((2 * TILE, TILE), jnp.bfloat16)
        acc = None
        for p in range(NB // 2):
            e, f = code_ref[i, 2 * p], code_ref[i, 2 * p + 1]
            v = jnp.concatenate([kv_out[e // 256, 1], kv_out[f // 256, 1]], axis=0)
            share_p = jnp.dot(
                p_bufs[b][:, p * 256:(p + 1) * 256],
                jnp.concatenate([v, ones], axis=1),
                preferred_element_type=jnp.float32,
            )
            acc = share_p if acc is None else acc + share_p
        o_ref[n] = (acc[:, :HD] / acc[:, HD:]).astype(jnp.bfloat16)

    base = len(live)

    def describe(k, source, target, device):
        return pltpu.make_async_remote_copy(
            src_ref=source,
            dst_ref=target,
            send_sem=send_sem.at[base + k],
            recv_sem=recv_sem.at[base + k],
            device_id=device,
            device_id_type=MESH,
        )

    hops = [
        describe(h, o_ref.at[pl.ds(h * half, half)], hop.at[h], z_dev[1 + h]) for h in range(2)
    ]
    ends = [
        describe(2 + h, o_ref.at[pl.ds((1 + h) * tiles, tiles)], got.at[1 - h], z_dev[1 + h])
        for h in range(2)
    ]
    last = [
        describe(4 + h, hop.at[h], got.at[2, pl.ds(h * half, half)], z_dev[1 + h]) for h in range(2)
    ]

    scores(jnp.int32(0), 0)
    scores(jnp.int32(1), 1)
    weights(0)

    def pair(k, carry):
        for r in range(2):
            n = 2 * k + r
            values(n, r)
            scores(n + 2, r)
            weights(1 - r)

        @pl.when(k == 1)
        def _():
            seen[...] = o_ref[2:4]

        @pl.when(k == 1)
        def _():
            for c in hops:
                c.start()

        @pl.when(k == 3)
        def _():
            seen[...] = o_ref[6:8]

        @pl.when(k == 3)
        def _():
            ends[0].start()

        @pl.when(k == 4)
        def _():
            for c, d in zip(hops, last):
                c.wait_recv()
                d.start()

        @pl.when(k == 5)
        def _():
            seen[...] = o_ref[10:12]

        @pl.when(k == 5)
        def _():
            ends[1].start()

        return carry

    lax.fori_loop(0, count // 2 - 1, pair, 0)
    values(jnp.int32(count - 2), 0)
    weights(1)
    values(jnp.int32(count - 1), 1)

    def add_head(pz, piece):
        o = piece.reshape(tiles * TILE, HD)
        w = wo_ref[pl.ds(pl.multiple_of(pz * HD, HD), HD), :]
        return jnp.dot(o, w, preferred_element_type=jnp.float32)

    for c in loads[7:]:
        c.wait()
    res_ref[...] = x_ref[...].astype(jnp.float32) + add_head(z, o_ref[3 * tiles:])
    for c in last:
        c.wait_recv()
    res_ref[...] += add_head(z_at[3], got[2])
    for h in (1, 0):
        ends[1 - h].wait_recv()
        res_ref[...] += add_head(z_at[1 + h], got[h])
    r = res_ref[...]
    inverse = lax.rsqrt(jnp.mean(r * r, axis=-1, keepdims=True) + 1e-06)
    norm_ref[...] = (r * inverse).astype(jnp.bfloat16)
    width = 256
    broad = 512

    def hidden(f, carry):
        cols = pl.ds(pl.multiple_of(f * broad, broad), broad)
        gate = jnp.dot(norm_ref[...], wg_ref[:, cols], preferred_element_type=jnp.float32)
        lift = jnp.dot(norm_ref[...], wu_ref[:, cols], preferred_element_type=jnp.float32)
        hid_ref[:, cols] = (gate / (1.0 + jnp.exp(-gate)) * lift).astype(jnp.bfloat16)
        return carry

    lax.fori_loop(0, wg_ref.shape[1] // broad, hidden, 0)

    def lower(f, carry):
        cols = pl.ds(pl.multiple_of(f * width, width), width)
        out_ref[:, cols] = (
            res_ref[:, cols]
            + jnp.dot(hid_ref[...], wd_ref[:, cols], preferred_element_type=jnp.float32)
        ).astype(jnp.bfloat16)
        return carry

    lax.fori_loop(0, D // width, lower, 0)
    for c in live + hops + ends + last:
        c.wait_send()


def body(
    x, lists, counts, valid, w_query, w_key, w_value, w_out, w_gate, w_up, w_down
):
    tiles = x.shape[0] // TILE
    piece = (tiles, 2, TILE, HD)
    weights = (w_query, w_key, w_value, w_out, w_gate, w_up, w_down)
    copied = (x,) + weights

    def fast(shape, dtype=x.dtype):
        return pltpu.VMEM(shape, dtype)

    return pl.pallas_call(
        layer_kernel,
        out_shape=jax.ShapeDtypeStruct(x.shape, x.dtype),
        in_specs=[pl.BlockSpec(memory_space=pltpu.HBM)] * 11,
        out_specs=pl.BlockSpec(memory_space=pltpu.VMEM),
        scratch_shapes=[
            fast(lists.shape, jnp.int32),
            pltpu.SMEM(counts.shape, jnp.int32),
            pltpu.SMEM(valid.shape, jnp.int32),
        ]
        + [fast(a.shape) for a in copied]
        + [
            fast((6 * 2 * ZD * tiles,) + piece[1:]),
            fast((ZD, tiles, TILE, HD)),
            fast((HEADS,) + piece),
            fast((HEADS, tiles, TILE, HD)),
            fast((8, 128), jnp.int32),
            fast((ZD, 8, 128), jnp.int32),
            fast((PARTS, tiles // PARTS) + piece[1:]),
            fast((len(DIRECT), tiles // PARTS) + piece[1:]),
            fast((ZD * tiles, 128), jnp.int32),
            pltpu.SMEM((ZD * tiles, 128), jnp.int32),
        ]
        + [fast((TILE, NB * TILE), jnp.float32)] * 2
        + [fast((TILE, NB * TILE))] * 2
        + [fast((TILE, TILE), jnp.float32)] * 2
        + [
            fast((ZD * tiles, TILE, HD)),
            fast((2, TILE, HD)),
            fast((ZD - 1, tiles, TILE, HD)),
            fast((2, tiles // 2, TILE, HD)),
            fast(x.shape, jnp.float32),
            fast(x.shape),
            fast((x.shape[0], w_gate.shape[1])),
            pltpu.SemaphoreType.DMA((12,)),
            pltpu.SemaphoreType.DMA((COPIES,)),
            pltpu.SemaphoreType.DMA((COPIES,)),
        ],
        compiler_params=pltpu.CompilerParams(
            collective_id=0, has_side_effects=True, vmem_limit_bytes=67043328
        ),
    )(lists, counts, valid, x, *weights)


def solution(mesh):
    placed = (
        P(("zone", "dev"), None),
        P(("zone", "dev"), None),
        P(("zone", "dev")),
        P(),
        P(),
        P(),
        P(),
        P(),
        P(),
        P(),
        P(),
    )
    return jax.shard_map(
        body, mesh=mesh, in_specs=placed, out_specs=P(("zone", "dev"), None), check_vma=False
    )
```

```python
import heapq
import math

import jax
import jax.numpy as jnp
from jax import lax
from jax.experimental import pallas as pl
from jax.experimental.pallas import tpu as pltpu
from jax.sharding import PartitionSpec as P

D = 512
HEADS = 4
HD = 128
TILE = 128
NB = 32
ZD = 4
NEG = -1e30
EXP_SCALE = math.log2(math.e) / math.sqrt(HD)


MESH = pl.DeviceIdType.MESH
PARTS = 4
DIRECT = ((1, 0), (1, 1), (1, 2), (1, 3), (2, 0), (2, 2))
OPENING = (("own", 0), ("next", 1), ("next", 3), ("relay", 1), ("next", 2), ("relay", 2), ("own", 3), ("own", 2), ("next", 0), ("relay", 3), ("own", 1), ("relay", 0))
FAR_UP = ((0, 0), (1, 0), (1, 2), (2, 0), (2, 3), (3, 0), (3, 1), (3, 3))


COPIES = 212


def arrivals():
    unit, hop = 5.6 / PARTS, 3.1
    free, events, order = {}, [], []

    def send(now, key, link):
        free[link] = max(now, free.get(link, 0.0)) + unit
        heapq.heappush(events, (free[link] + hop, len(order) + len(events), key))

    def own(now, u):
        if u in DIRECT:
            send(now, ("transit", u), "back")
        else:
            send(now, ("below", u), "up")
            send(now, ("above", u), "down")

    for kind, h in OPENING:
        if kind == "own":
            own(0.0, (0, h))
        elif kind == "next":
            send(0.0, ("own", (2, h)), "next")
            send(0.0, ("own", (1, h)), "prior")
        else:
            send(0.0, ("relay", h), "next" if 2 * h < PARTS else "prior")
    while events:
        now, _, (kind, u) = heapq.heappop(events)
        order.append((kind, u))
        if kind == "own":
            own(now, u)
        elif kind == "relay":
            send(now, ("own", (3, u)), "next" if 2 * u < PARTS else "prior")
        elif kind == "transit":
            send(now, ("halo_below", u), "up")
            send(now, ("halo_above", u), "down")
        elif kind in ("above", "below"):
            if (kind == "below") == (u in FAR_UP):
                send(now, ("far", u), "up" if kind == "below" else "down")
            if u not in DIRECT:
                send(now, ("halo_" + kind, u), "halo")
        elif kind in ("halo_above", "halo_below") and u in DIRECT:
            send(now, (kind[5:], u), "back")
    return order


def layer_kernel(
    nb_hbm, count_hbm, valid_hbm, x_hbm, wq_hbm, wk_hbm, wv_hbm, wo_hbm, wg_hbm, wu_hbm, wd_hbm,
    out_ref,
    nb_ref, count_ref, valid_ref, x_ref, wq_ref, wk_ref, wv_ref, wo_ref, wg_ref, wu_ref, wd_ref,
    kv_out, q_out, kv_ref, q_ref, raw, raw_all, relay, transit, code_vec, code_ref,
    s_even, s_odd, p_even, p_odd, t_even, t_odd,
    o_ref, seen, got, hop, res_ref, norm_ref, hid_ref,
    load_sem, send_sem, recv_sem,
):
    zone, dev = lax.axis_index("zone"), lax.axis_index("dev")
    x, y_lo = zone // 2, zone % 2
    y_hi, z, core = dev // 8, (dev // 2) % ZD, dev % 2
    y = y_hi * 2 + y_lo
    tiles = x_ref.shape[0] // TILE
    size = tiles // PARTS
    half = tiles // 2

    def at(px, py, pz, pc):
        return (px * 2 + py % 2, (py // 2) * 8 + pz * 2 + pc)

    side = 1 - 2 * y_lo
    up, down = at(x, (y + 1) % 4, z, core), at(x, (y + 3) % 4, z, core)
    halo, back = at((x + 4 + side) % 4, y, z, core), at((x + 4 - side) % 4, y, z, core)
    partner = at(x, y, z, 1 - core)
    z_at = [(z + d) % ZD for d in (0, 1, 3, 2)]
    z_dev = [at(x, y, pz, core) for pz in z_at]

    barrier = pltpu.get_barrier_semaphore()
    peers = [up, down, halo, back, partner] + z_dev[1:]
    for peer in peers:
        pl.semaphore_signal(barrier, inc=1, device_id=peer, device_id_type=MESH)

    loads = [
        pltpu.make_async_copy(source, target, load_sem.at[i])
        for i, (source, target) in enumerate(
            (
                (x_hbm, x_ref), (wk_hbm, wk_ref), (wv_hbm, wv_ref), (nb_hbm, nb_ref),
                (count_hbm, count_ref), (wq_hbm, wq_ref), (valid_hbm, valid_ref),
                (wo_hbm, wo_ref), (wg_hbm, wg_ref), (wu_hbm, wu_ref), (wd_hbm, wd_ref),
            )
        )
    ]
    for c in loads:
        c.start()
    for c in loads[:5]:
        c.wait()

    lane = lax.broadcasted_iota(jnp.int32, (1, 128), 1)
    raw[...] = jnp.full(raw.shape, -1, jnp.int32)
    raw[:tiles, :NB] = nb_ref[...]
    for t in range(tiles):
        n = count_ref[t]
        row = jnp.where(lane < jnp.minimum(n, NB), raw[t:t + 1, :], -1)
        raw[t:t + 1, :] = jnp.where(lane == NB, n, row)

    def rows_of(t):
        return x_ref[pl.ds(pl.multiple_of(t * TILE, TILE), TILE), :]

    def keys_values(t, carry):
        rows = rows_of(t)
        k = jnp.dot(rows, wk_ref[...], preferred_element_type=jnp.float32)
        for h in range(HEADS):
            kv_ref[h, t, 0] = jnp.transpose(k[:, h * HD:(h + 1) * HD]).astype(jnp.bfloat16)
        v = jnp.dot(rows, wv_ref[...], preferred_element_type=jnp.float32).astype(jnp.bfloat16)
        for h in range(HEADS):
            kv_ref[h, t, 1] = v[:, h * HD:(h + 1) * HD]
        return carry

    lax.fori_loop(0, tiles, keys_values, 0)
    kv_out[pl.ds((core * ZD + z) * tiles, tiles)] = kv_ref[z]
    pl.semaphore_wait(barrier, len(peers))

    live, flying, shared = [], {}, []

    def send(source, target, device):
        k = len(live)
        copy = pltpu.make_async_remote_copy(
            src_ref=source,
            dst_ref=target,
            send_sem=send_sem.at[k],
            recv_sem=recv_sem.at[k],
            device_id=device,
            device_id_type=MESH,
        )
        copy.start()
        live.append(copy)
        return copy

    def part(h):
        return pl.ds(h * size, size)

    def spot_of(slot, pz, h):
        return kv_out.at[pl.ds(((slot * 2 + core) * ZD + pz) * tiles + h * size, size)]

    def place(slot, u):
        return spot_of(slot, z_at[u[0]], u[1])

    def share(slot, u, source=None):
        shared.append(send(place(slot, u) if source is None else source, place(slot, u), partner))

    def own(u, source):
        if u in DIRECT:
            flying["transit", u] = send(source, transit.at[DIRECT.index(u)], back)
        else:
            flying["below", u] = send(source, place(2, u), up)
            flying["above", u] = send(source, place(1, u), down)
        share(0, u, source)

    def forward(kind, u):
        flying[kind, u].wait_recv()
        if kind == "own":
            own(u, place(0, u))
        elif kind == "relay":
            along = 2 * u < PARTS
            flying["own", (3, u)] = send(
                relay.at[u], spot_of(0, z_at[2 if along else 1], u), z_dev[1 if along else 2]
            )
        elif kind == "transit":
            spot = transit.at[DIRECT.index(u)]
            flying["halo_below", u] = send(spot, place(5, u), up)
            flying["halo_above", u] = send(spot, place(4, u), down)
        elif kind in ("above", "below"):
            slot = 1 if kind == "above" else 2
            if (kind == "below") == (u in FAR_UP):
                flying["far", u] = send(
                    place(slot, u), place(3, u), up if kind == "below" else down
                )
            if u not in DIRECT:
                flying["halo_" + kind, u] = send(place(slot, u), place(slot + 3, u), halo)
            share(slot, u)
        elif kind == "far":
            share(3, u)
        else:
            slot = 4 if kind == "halo_above" else 5
            if u in DIRECT:
                flying[kind[5:], u] = send(place(slot, u), place(slot - 3, u), back)
            share(slot, u)

    for kind, h in OPENING:
        if kind == "own":
            own((0, h), kv_ref.at[z, part(h)])
        elif kind == "next":
            flying["own", (2, h)] = send(
                kv_ref.at[z_at[1], part(h)], spot_of(0, z, h), z_dev[1]
            )
            flying["own", (1, h)] = send(
                kv_ref.at[z_at[2], part(h)], spot_of(0, z, h), z_dev[2]
            )
        else:
            flying["relay", h] = send(
                kv_ref.at[z_at[3], part(h)], relay.at[h], z_dev[1 if 2 * h < PARTS else 2]
            )

    def queries(t, carry):
        q = jnp.dot(rows_of(t), wq_ref[...], preferred_element_type=jnp.float32)
        q = q.astype(jnp.bfloat16)
        for h in range(HEADS):
            q_ref[h, t] = q[:, h * HD:(h + 1) * HD]
        return carry

    loads[5].wait()
    lax.fori_loop(0, tiles, queries, 0)
    q_out[z] = q_ref[z]
    raw_all[z] = raw[...]

    order = arrivals()
    relays = [n for n, (kind, _) in enumerate(order) if kind == "relay"]
    middle = 2 * len(order) // 3
    for kind, u in order[:relays[-1] + 1]:
        forward(kind, u)
    q_in, raw_in = {}, {}
    for j, lands in ((1, 2), (2, 1), (3, 3)):
        raw_in[lands] = send(raw, raw_all.at[z], z_dev[j])
        q_in[lands] = send(q_ref.at[z_at[j]], q_out.at[z], z_dev[j])
    for kind, u in order[relays[-1] + 1:middle]:
        forward(kind, u)

    for j in (1, 2, 3):
        raw_in[j].wait_recv()
    lists = raw_all[...].reshape(ZD * raw.shape[0], 128)

    loads[6].wait()

    span = 3 * 64

    def look_up(i, found):
        g = (zone * 64 + valid_ref.shape[0] - 64 + i) % valid_ref.shape[0]
        return jnp.where(lists == g, valid_ref[g], found)

    found = lax.fori_loop(0, span, look_up, jnp.zeros_like(lists), unroll=8)
    spot = jnp.maximum(lists, 0)
    relative = (spot // 64 + 9 - zone) % 8
    there_y = (spot // 32) % 2 * 2 + 1 - y_lo
    near = jnp.where((there_y + 4 - y) % 4 == 1, 1, 2)
    near = near + jnp.where(relative == 2 - 2 * y_lo, 0, 3)
    slot = jnp.where(relative == 1, jnp.where((spot // 32) % 2 == y_hi, 0, 3), near)
    code = ((slot * 2 + (spot // 4) % 2) * ZD + (spot // 8) % ZD) * 4 + spot % 4
    code = jnp.where(lists < 0, 0, code * 256 + found)
    code = jnp.where(lane == NB, lists, code)
    for p in range(ZD):
        code_vec[p * tiles:(p + 1) * tiles, :] = code[p * raw.shape[0]:p * raw.shape[0] + tiles]

    to_smem = pltpu.make_async_copy(code_vec, code_ref, load_sem.at[11])
    to_smem.start()
    for kind, u in order[middle:]:
        forward(kind, u)
    for c in shared + list(q_in.values()):
        c.wait_recv()
    to_smem.wait()

    s_bufs, p_bufs = (s_even, s_odd), (p_even, p_odd)
    t_bufs = (t_even, t_odd)
    count = ZD * tiles

    def owner(n):
        g = n // tiles
        d = jnp.where(g == 0, 2, jnp.where(g == 1, 1, jnp.where(g == 2, 3, 0)))
        return (z + d) % ZD

    def scores(n, b):
        pz, t = owner(n), n % tiles
        i = pz * tiles + t
        q = q_out[pz, t]
        top = None
        for p in range(NB // 2):
            e, f = code_ref[i, 2 * p], code_ref[i, 2 * p + 1]
            keys = jnp.concatenate([kv_out[e // 256, 0], kv_out[f // 256, 0]], axis=1)
            s = jnp.dot(q, keys, preferred_element_type=jnp.float32)
            bias = jnp.concatenate(
                [jnp.where(lane < e % 256, 0.0, NEG), jnp.where(lane < f % 256, 0.0, NEG)],
                axis=1,
            )
            s = s + bias
            s_bufs[b][:, p * 256:(p + 1) * 256] = s
            pair_top = jnp.maximum(s[:, :TILE], s[:, TILE:])
            top = pair_top if top is None else jnp.maximum(top, pair_top)
        t_bufs[b][...] = top

    def weights(b):
        for g in range(TILE // 16):
            rows = slice(g * 16, (g + 1) * 16)
            peak = jnp.max(t_bufs[b][rows, :], axis=1, keepdims=True)
            for k in range(NB):
                cols = slice(k * TILE, (k + 1) * TILE)
                w = jnp.exp2((s_bufs[b][rows, cols] - peak) * EXP_SCALE)
                p_bufs[b][rows, cols] = w.astype(jnp.bfloat16)

    def values(n, b):
        i = owner(n) * tiles + n % tiles
        ones = jnp.ones((2 * TILE, TILE), jnp.bfloat16)
        acc = None
        for p in range(NB // 2):
            e, f = code_ref[i, 2 * p], code_ref[i, 2 * p + 1]
            v = jnp.concatenate([kv_out[e // 256, 1], kv_out[f // 256, 1]], axis=0)
            share_p = jnp.dot(
                p_bufs[b][:, p * 256:(p + 1) * 256],
                jnp.concatenate([v, ones], axis=1),
                preferred_element_type=jnp.float32,
            )
            acc = share_p if acc is None else acc + share_p
        o_ref[n] = (acc[:, :HD] / acc[:, HD:]).astype(jnp.bfloat16)

    base = len(live)

    def describe(k, source, target, device):
        return pltpu.make_async_remote_copy(
            src_ref=source,
            dst_ref=target,
            send_sem=send_sem.at[base + k],
            recv_sem=recv_sem.at[base + k],
            device_id=device,
            device_id_type=MESH,
        )

    hops = [
        describe(h, o_ref.at[pl.ds(h * half, half)], hop.at[h], z_dev[1 + h]) for h in range(2)
    ]
    ends = [
        describe(2, o_ref.at[pl.ds(tiles, tiles)], got.at[1], z_dev[1]),
        describe(3, o_ref.at[pl.ds(2 * tiles, half)], got.at[0, pl.ds(0, half)], z_dev[2]),
        describe(6, o_ref.at[pl.ds(2 * tiles + half, half)], got.at[0, pl.ds(half, half)], z_dev[2]),
    ]
    last = [
        describe(4 + h, hop.at[h], got.at[2, pl.ds(h * half, half)], z_dev[1 + h]) for h in range(2)
    ]

    scores(jnp.int32(0), 0)
    scores(jnp.int32(1), 1)
    weights(0)

    def pair(k, carry):
        for r in range(2):
            n = 2 * k + r
            values(n, r)
            scores(n + 2, r)
            weights(1 - r)

        @pl.when(k == 1)
        def _():
            seen[...] = o_ref[2:4]

        @pl.when(k == 1)
        def _():
            for c in hops:
                c.start()

        @pl.when(k == 3)
        def _():
            seen[...] = o_ref[6:8]

        @pl.when(k == 3)
        def _():
            ends[0].start()

        @pl.when(k == 4)
        def _():
            for c, d in zip(hops, last):
                c.wait_recv()
                d.start()
            seen[...] = o_ref[8:10]

        @pl.when(k == 4)
        def _():
            ends[1].start()

        @pl.when(k == 5)
        def _():
            seen[...] = o_ref[10:12]

        @pl.when(k == 5)
        def _():
            ends[2].start()

        return carry

    lax.fori_loop(0, count // 2 - 1, pair, 0)
    values(jnp.int32(count - 2), 0)
    weights(1)
    values(jnp.int32(count - 1), 1)

    def add_head(pz, piece):
        o = piece.reshape(tiles * TILE, HD)
        w = wo_ref[pl.ds(pl.multiple_of(pz * HD, HD), HD), :]
        return jnp.dot(o, w, preferred_element_type=jnp.float32)

    for c in loads[7:]:
        c.wait()
    res_ref[...] = x_ref[...].astype(jnp.float32) + add_head(z, o_ref[3 * tiles:])
    for c in last:
        c.wait_recv()
    res_ref[...] += add_head(z_at[3], got[2])
    ends[0].wait_recv()
    res_ref[...] += add_head(z_at[2], got[1])
    ends[1].wait_recv()
    ends[2].wait_recv()
    res_ref[...] += add_head(z_at[1], got[0])
    r = res_ref[...]
    inverse = lax.rsqrt(jnp.mean(r * r, axis=-1, keepdims=True) + 1e-06)
    norm_ref[...] = (r * inverse).astype(jnp.bfloat16)
    width = 256
    broad = 512

    def hidden(f, carry):
        cols = pl.ds(pl.multiple_of(f * broad, broad), broad)
        gate = jnp.dot(norm_ref[...], wg_ref[:, cols], preferred_element_type=jnp.float32)
        lift = jnp.dot(norm_ref[...], wu_ref[:, cols], preferred_element_type=jnp.float32)
        hid_ref[:, cols] = (gate / (1.0 + jnp.exp(-gate)) * lift).astype(jnp.bfloat16)
        return carry

    lax.fori_loop(0, wg_ref.shape[1] // broad, hidden, 0)

    def lower(f, carry):
        cols = pl.ds(pl.multiple_of(f * width, width), width)
        out_ref[:, cols] = (
            res_ref[:, cols]
            + jnp.dot(hid_ref[...], wd_ref[:, cols], preferred_element_type=jnp.float32)
        ).astype(jnp.bfloat16)
        return carry

    lax.fori_loop(0, D // width, lower, 0)
    for c in live + hops + ends + last:
        c.wait_send()


def body(
    x, lists, counts, valid, w_query, w_key, w_value, w_out, w_gate, w_up, w_down
):
    tiles = x.shape[0] // TILE
    piece = (tiles, 2, TILE, HD)
    weights = (w_query, w_key, w_value, w_out, w_gate, w_up, w_down)
    copied = (x,) + weights

    def fast(shape, dtype=x.dtype):
        return pltpu.VMEM(shape, dtype)

    return pl.pallas_call(
        layer_kernel,
        out_shape=jax.ShapeDtypeStruct(x.shape, x.dtype),
        in_specs=[pl.BlockSpec(memory_space=pltpu.HBM)] * 11,
        out_specs=pl.BlockSpec(memory_space=pltpu.VMEM),
        scratch_shapes=[
            fast(lists.shape, jnp.int32),
            pltpu.SMEM(counts.shape, jnp.int32),
            pltpu.SMEM(valid.shape, jnp.int32),
        ]
        + [fast(a.shape) for a in copied]
        + [
            fast((6 * 2 * ZD * tiles,) + piece[1:]),
            fast((ZD, tiles, TILE, HD)),
            fast((HEADS,) + piece),
            fast((HEADS, tiles, TILE, HD)),
            fast((8, 128), jnp.int32),
            fast((ZD, 8, 128), jnp.int32),
            fast((PARTS, tiles // PARTS) + piece[1:]),
            fast((len(DIRECT), tiles // PARTS) + piece[1:]),
            fast((ZD * tiles, 128), jnp.int32),
            pltpu.SMEM((ZD * tiles, 128), jnp.int32),
        ]
        + [fast((TILE, NB * TILE), jnp.float32)] * 2
        + [fast((TILE, NB * TILE))] * 2
        + [fast((TILE, TILE), jnp.float32)] * 2
        + [
            fast((ZD * tiles, TILE, HD)),
            fast((2, TILE, HD)),
            fast((ZD - 1, tiles, TILE, HD)),
            fast((2, tiles // 2, TILE, HD)),
            fast(x.shape, jnp.float32),
            fast(x.shape),
            fast((x.shape[0], w_gate.shape[1])),
            pltpu.SemaphoreType.DMA((12,)),
            pltpu.SemaphoreType.DMA((COPIES,)),
            pltpu.SemaphoreType.DMA((COPIES,)),
        ],
        compiler_params=pltpu.CompilerParams(
            collective_id=0, has_side_effects=True, vmem_limit_bytes=67043328
        ),
    )(lists, counts, valid, x, *weights)


def solution(mesh):
    placed = (
        P(("zone", "dev"), None),
        P(("zone", "dev"), None),
        P(("zone", "dev")),
        P(),
        P(),
        P(),
        P(),
        P(),
        P(),
        P(),
        P(),
    )
    return jax.shard_map(
        body, mesh=mesh, in_specs=placed, out_specs=P(("zone", "dev"), None), check_vma=False
    )
```
